256 devices in a mesh: nodes: 128 (over z, x, y), feat: 2 (over core).
Axes of the slice: x: 4, y: 4, z: 8, core: 2. Of those that a mesh axis runs over, the one named last changes fastest.
Arguments:
- grid_latent: bfloat16 [131072, 512], P('nodes', 'feat'), may hold values from -6 to 6
- mesh_latent: bfloat16 [131072, 512], P('nodes', 'feat'), may hold values from -6 to 6
- grid_order: int32 [128, 1024], P('nodes'), may hold values from 0 to 1023, each once within a row
- enc_send_block: int32 [2048], P('nodes'), may hold values from 0 to 7
- enc_recv_block: int32 [2048], P('nodes'), may hold values from 0 to 7
- enc_offsets: int32 [2048, 2, 128], P('nodes'), may hold values from 0 to 127
- enc_classes: int32 [2048, 128], P('nodes'), may hold values from 0 to 7
- enc_live: int32 [128], P('nodes'), may hold values from 1 to 16, 1280 in all
- mesh_send_block: int32 [12288], P('nodes'), may hold values from 0 to 23
- mesh_recv_block: int32 [12288], P('nodes'), may hold values from 0 to 7
- mesh_offsets: int32 [12288, 2, 128], P('nodes'), may hold values from 0 to 127
- mesh_classes: int32 [12288, 128], P('nodes'), may hold values from 0 to 7
- mesh_live: int32 [128], P('nodes'), may hold values from 1 to 96, 7680 in all
- dec_send_block: int32 [3072], P('nodes'), may hold values from 0 to 7
- dec_recv_block: int32 [3072], P('nodes'), may hold values from 0 to 7
- dec_offsets: int32 [3072, 2, 128], P('nodes'), may hold values from 0 to 127
- dec_classes: int32 [3072, 128], P('nodes'), may hold values from 0 to 7
- dec_live: int32 [128], P('nodes'), may hold values from 1 to 24, 1920 in all
- class_gain: float32 [3, 8], replicated, may hold values from 0.25 to 2
- enc_weights: bfloat16 [3, 512, 512], P(None, None, 'feat'), may hold values from -0.25 to 0.25
- mesh_weights: bfloat16 [2, 3, 512, 512], P(None, None, None, 'feat'), may hold values from -0.25 to 0.25
- dec_weights: bfloat16 [3, 512, 512], P(None, None, 'feat'), may hold values from -0.25 to 0.25
- enc_bias: float32 [512], P('feat'), may hold values from -3 to 3
- enc_gain: float32 [512], P('feat'), may hold values from 0.25 to 1.75
- mesh_bias: float32 [2, 512], P(None, 'feat'), may hold values from -3 to 3
- mesh_gain: float32 [2, 512], P(None, 'feat'), may hold values from 0.25 to 1.75
- dec_bias: float32 [512], P('feat'), may hold values from -3 to 3
- dec_gain: float32 [512], P('feat'), may hold values from 0.25 to 1.75
Outputs:
- grid_out: bfloat16 [131072, 512], P('nodes', 'feat')
- mesh_final: bfloat16 [131072, 512], P('nodes', 'feat')
The draws below stay inside these ranges and needn't reach their ends.
Inputs may be any that keep to these rules, and one draw needn't show every extreme that they name: Each row of grid_order lists each of 0..1023 once. The first enc_live[d] edge blocks of region d are live; the most is reached on some region. The first mesh_live[d] edge blocks of region d are live; the most is reached on some region. The first dec_live[d] edge blocks of region d are live; the most is reached on some region.
All inputs are finite; a program needn't handle non-finite values.
Results may differ from the reference program's by a relative error of at most 0.0085.
Values may be sent and summed in bfloat16 or wider, within the bound.
A program may use at most 64 MiB of HBM per device.

```python
import math
import jax
import jax.numpy as jnp
import numpy as np
from jax import lax

D = 512
GRID_DEV = 1024
MESH_DEV = 1024
BLOCK = 128
ROUNDS = 2
NCLASS = 8
GRID = 131072
MESH = 131072
EB_ENC = 16
EB_MESH = 96
EB_DEC = 24
N_NODES = 128


def plant(array, rng, least, high):
    longest = array.shape.index(max(array.shape))
    spots = []
    for shift in (0, 1):
        where = [jax.random.randint(jax.random.fold_in(rng, axis), (), 0, length) for axis, length in enumerate(array.shape)]
        where[longest] = (where[longest] + shift) % array.shape[longest]
        spots.append(tuple(where))
    return array.at[spots[0]].set(least).at[spots[1]].set(high)


def steps_of(stream_key, shape, cuts, least, top_value):
    def one(position, blocks):
        heights = jax.random.uniform(jax.random.fold_in(jax.random.fold_in(stream_key, 6), position), (blocks,), jnp.float32, least / len(cuts), top_value / len(cuts))
        return jnp.repeat(jnp.exp(heights), shape[position] // blocks).reshape((-1,) + (1,) * (len(shape) - position - 1))

    gain = one(*cuts[0])
    for cut in cuts[1:]:
        gain = gain * one(*cut)
    return gain


def length_profile(amount, total, most, skew):
    loads = [(1 << 20) // math.isqrt(rank ** skew) + 1 for rank in range(2, amount + 1)]
    surplus, given = total - most - (amount - 1), [1] * (amount - 1)
    while surplus > 0:
        candidates = [i for i in range(amount - 1) if given[i] < most]
        whole, left = sum([loads[i] for i in candidates]), surplus
        for i in candidates:
            addition = min(most - given[i], max(1, left * loads[i] // whole), surplus)
            given[i] = given[i] + addition
            surplus = surplus - addition
    return np.array([most] + given)


def ragged_sizes(key, amount, total, limit, slope):
    if amount == 2:
        one = jax.random.randint(key, (), max(1, total - limit), min(limit, total - 1) + 1)
        return jnp.stack([one, total - one])
    lengths = jnp.asarray(length_profile(amount, total, limit, slope), jnp.int32)
    couples = (amount - 1) // 2
    source_of, sink = lengths[1:1 + 2 * couples:2], lengths[2:2 + 2 * couples:2]
    room = jnp.minimum(source_of - 1, limit - sink)
    shifted = jax.random.randint(jax.random.fold_in(key, 1), (couples,), 0, 1 << 20) % (room + 1)
    lengths = lengths.at[1:1 + 2 * couples:2].set(source_of - shifted).at[2:2 + 2 * couples:2].set(sink + shifted)
    return lengths[jax.random.permutation(jax.random.fold_in(key, 2), amount)]


def bell_draw(own_key, extent, width, most, cuts=(), held_as=jnp.bfloat16):
    entries = width * jax.random.normal(own_key, extent, jnp.float32)
    if cuts:
        entries = entries * steps_of(own_key, extent, cuts, -0.22, 0.18)
    return jnp.clip(entries, -most, most).astype(held_as)


def setup_inputs(seed: int = 0) -> dict:
    keys = jax.random.split(jax.random.key(seed), 29)
    grid_latent = bell_draw(keys[0], (GRID, D), 1.0, 6.0, ((0, 128), (1, 2)))
    mesh_latent = bell_draw(keys[1], (MESH, D), 1.0, 6.0, ((0, 128), (1, 2)))
    grid_order = jax.vmap(lambda own: jax.random.permutation(own, GRID_DEV))(jax.random.split(keys[2], N_NODES)).reshape((N_NODES, GRID_DEV)).astype(jnp.int32)
    enc_send_block = plant(jax.random.randint(keys[3], (N_NODES * EB_ENC,), 0, GRID_DEV // BLOCK), jax.random.fold_in(keys[3], 1), 0, (GRID_DEV // BLOCK) - 1).astype(jnp.int32)
    enc_recv_block = plant(jax.random.randint(keys[4], (N_NODES * EB_ENC,), 0, MESH_DEV // BLOCK), jax.random.fold_in(keys[4], 1), 0, (MESH_DEV // BLOCK) - 1).astype(jnp.int32)
    enc_offsets = plant(jax.random.randint(keys[5], (N_NODES * EB_ENC, 2, BLOCK), 0, BLOCK), jax.random.fold_in(keys[5], 1), 0, BLOCK - 1).astype(jnp.int32)
    enc_classes = plant(jax.random.randint(keys[6], (N_NODES * EB_ENC, BLOCK), 0, NCLASS), jax.random.fold_in(keys[6], 1), 0, NCLASS - 1).astype(jnp.int32)
    enc_live = ragged_sizes(keys[7], N_NODES, N_NODES * EB_ENC * 5 // 8, EB_ENC, 2).astype(jnp.int32)
    mesh_send_block = plant(jax.random.randint(keys[8], (N_NODES * EB_MESH,), 0, 3 * MESH_DEV // BLOCK), jax.random.fold_in(keys[8], 1), 0, (3 * MESH_DEV // BLOCK) - 1).astype(jnp.int32)
    mesh_recv_block = plant(jax.random.randint(keys[9], (N_NODES * EB_MESH,), 0, MESH_DEV // BLOCK), jax.random.fold_in(keys[9], 1), 0, (MESH_DEV // BLOCK) - 1).astype(jnp.int32)
    mesh_offsets = plant(jax.random.randint(keys[10], (N_NODES * EB_MESH, 2, BLOCK), 0, BLOCK), jax.random.fold_in(keys[10], 1), 0, BLOCK - 1).astype(jnp.int32)
    mesh_classes = plant(jax.random.randint(keys[11], (N_NODES * EB_MESH, BLOCK), 0, NCLASS), jax.random.fold_in(keys[11], 1), 0, NCLASS - 1).astype(jnp.int32)
    mesh_live = ragged_sizes(keys[12], N_NODES, N_NODES * EB_MESH * 5 // 8, EB_MESH, 2).astype(jnp.int32)
    dec_send_block = plant(jax.random.randint(keys[13], (N_NODES * EB_DEC,), 0, MESH_DEV // BLOCK), jax.random.fold_in(keys[13], 1), 0, (MESH_DEV // BLOCK) - 1).astype(jnp.int32)
    dec_recv_block = plant(jax.random.randint(keys[14], (N_NODES * EB_DEC,), 0, GRID_DEV // BLOCK), jax.random.fold_in(keys[14], 1), 0, (GRID_DEV // BLOCK) - 1).astype(jnp.int32)
    dec_offsets = plant(jax.random.randint(keys[15], (N_NODES * EB_DEC, 2, BLOCK), 0, BLOCK), jax.random.fold_in(keys[15], 1), 0, BLOCK - 1).astype(jnp.int32)
    dec_classes = plant(jax.random.randint(keys[16], (N_NODES * EB_DEC, BLOCK), 0, NCLASS), jax.random.fold_in(keys[16], 1), 0, NCLASS - 1).astype(jnp.int32)
    dec_live = ragged_sizes(keys[17], N_NODES, N_NODES * EB_DEC * 5 // 8, EB_DEC, 2).astype(jnp.int32)
    class_gain = jnp.clip(jnp.exp(jax.random.uniform(keys[18], (3, NCLASS), jnp.float32, math.log(0.25), math.log(2.0))), 0.25, 2.0)
    enc_weights = bell_draw(keys[19], (3, D, D), D ** -0.5, 0.25, ((2, 2),))
    mesh_weights = bell_draw(keys[20], (ROUNDS, 3, D, D), D ** -0.5, 0.25, ((3, 2),))
    dec_weights = bell_draw(keys[21], (3, D, D), D ** -0.5, 0.25, ((2, 2),))
    enc_bias = bell_draw(keys[22], (D,), 0.5, 3.0, ((0, 2),), jnp.float32)
    enc_gain = jnp.clip(1.0 + 0.15 * jax.random.normal(keys[23], (D,), jnp.float32), 0.25, 1.75)
    mesh_bias = bell_draw(keys[24], (ROUNDS, D), 0.5, 3.0, ((1, 2),), jnp.float32)
    mesh_gain = jnp.clip(1.0 + 0.15 * jax.random.normal(keys[25], (ROUNDS, D), jnp.float32), 0.25, 1.75)
    dec_bias = bell_draw(keys[26], (D,), 0.5, 3.0, ((0, 2),), jnp.float32)
    dec_gain = jnp.clip(1.0 + 0.15 * jax.random.normal(keys[27], (D,), jnp.float32), 0.25, 1.75)
    return {"grid_latent": grid_latent, "mesh_latent": mesh_latent, "grid_order": grid_order, "enc_send_block": enc_send_block, "enc_recv_block": enc_recv_block, "enc_offsets": enc_offsets, "enc_classes": enc_classes, "enc_live": enc_live, "mesh_send_block": mesh_send_block, "mesh_recv_block": mesh_recv_block, "mesh_offsets": mesh_offsets, "mesh_classes": mesh_classes, "mesh_live": mesh_live, "dec_send_block": dec_send_block, "dec_recv_block": dec_recv_block, "dec_offsets": dec_offsets, "dec_classes": dec_classes, "dec_live": dec_live, "class_gain": class_gain, "enc_weights": enc_weights, "mesh_weights": mesh_weights, "dec_weights": dec_weights, "enc_bias": enc_bias, "enc_gain": enc_gain, "mesh_bias": mesh_bias, "mesh_gain": mesh_gain, "dec_bias": dec_bias, "dec_gain": dec_gain}


epsilon = 1e-05

def project(inputs, matrix):
    return jnp.dot(inputs, matrix, preferred_element_type=jnp.float32)

def normed(mixed, gain_vector):
    average = lax.optimization_barrier(jnp.mean(mixed, axis=-1, keepdims=True))
    spread = lax.optimization_barrier(jnp.mean(mixed * mixed, axis=-1, keepdims=True)) - average * average
    return (mixed - average) * lax.rsqrt(spread + epsilon) * gain_vector

def edge_sum(sender, receiver, bias_row, class_row, send_ids, recv_ids, offset_pair, labels, live_count, row_count):
    slots = send_ids.shape[0]
    sender_rows = send_ids[:, None] * BLOCK + offset_pair[:, 0, :]
    taker_rows = recv_ids[:, None] * BLOCK + offset_pair[:, 1, :]
    living = (jnp.arange(slots, dtype=jnp.int32) < live_count).astype(jnp.float32)
    weight = class_row[labels] * living[:, None]
    summed = sender[sender_rows].astype(jnp.float32) + receiver[taker_rows].astype(jnp.float32) + bias_row
    message = (jax.nn.silu(summed) * weight[:, :, None]).astype(jnp.bfloat16)
    flat = message.reshape(-1, message.shape[-1]).astype(jnp.float32)
    return jax.ops.segment_sum(flat, taker_rows.reshape(-1), num_segments=row_count)

def refresh(residual, gathered, matrix, gain_vector):
    mixed = project(gathered.reshape(-1, D).astype(jnp.bfloat16), matrix)
    return (residual.astype(jnp.float32) + normed(mixed, gain_vector)).astype(jnp.bfloat16)

def reference(grid_latent, mesh_latent, grid_order, enc_send_block, enc_recv_block, enc_offsets, enc_classes, enc_live, mesh_send_block, mesh_recv_block, mesh_offsets, mesh_classes, mesh_live, dec_send_block, dec_recv_block, dec_offsets, dec_classes, dec_live, class_gain, enc_weights, mesh_weights, dec_weights, enc_bias, enc_gain, mesh_bias, mesh_gain, dec_bias, dec_gain):
    node_count = N_NODES
    per_peer = GRID_DEV // node_count
    routing = grid_order.reshape(node_count, node_count, per_peer) + (jnp.arange(node_count, dtype=jnp.int32) * GRID_DEV)[:, None, None]
    received = jnp.transpose(routing, (1, 0, 2)).reshape(node_count, GRID_DEV)
    send_proj = project(grid_latent, enc_weights[0]).astype(jnp.bfloat16)
    grid_proj = project(grid_latent, dec_weights[1]).astype(jnp.bfloat16)
    mesh_proj = project(mesh_latent, enc_weights[1]).astype(jnp.bfloat16).reshape(node_count, MESH_DEV, D)

    def encode(pieces):
        rows_index, receiver, send_ids, recv_ids, offset_pair, labels, live_count = pieces
        return edge_sum(send_proj[rows_index], receiver, enc_bias, class_gain[0], send_ids, recv_ids, offset_pair, labels, live_count, MESH_DEV)
    enc_agg = lax.map(encode, (received, mesh_proj, enc_send_block.reshape(node_count, -1), enc_recv_block.reshape(node_count, -1), enc_offsets.reshape(node_count, -1, 2, BLOCK), enc_classes.reshape(node_count, -1, BLOCK), enc_live))
    mesh = refresh(mesh_latent, enc_agg, enc_weights[2], enc_gain)
    for round_index in range(ROUNDS):
        weights = mesh_weights[round_index]
        round_bias = mesh_bias[round_index]
        sending = project(mesh, weights[0]).astype(jnp.bfloat16).reshape(node_count, MESH_DEV, D)
        taking = project(mesh, weights[1]).astype(jnp.bfloat16).reshape(node_count, MESH_DEV, D)
        nearby = jnp.concatenate([jnp.roll(sending, 1, axis=0), sending, jnp.roll(sending, -1, axis=0)], axis=1)

        def relay(pieces):
            sender, receiver, send_ids, recv_ids, offset_pair, labels, live_count = pieces
            return edge_sum(sender, receiver, round_bias, class_gain[1], send_ids, recv_ids, offset_pair, labels, live_count, MESH_DEV)
        mesh_agg = lax.map(relay, (nearby, taking, mesh_send_block.reshape(node_count, -1), mesh_recv_block.reshape(node_count, -1), mesh_offsets.reshape(node_count, -1, 2, BLOCK), mesh_classes.reshape(node_count, -1, BLOCK), mesh_live))
        mesh = refresh(mesh, mesh_agg, weights[2], mesh_gain[round_index])
    dec_proj = project(mesh, dec_weights[0]).astype(jnp.bfloat16).reshape(node_count, MESH_DEV, D)

    def decode(pieces):
        rows_index, sender, send_ids, recv_ids, offset_pair, labels, live_count = pieces
        return edge_sum(sender, grid_proj[rows_index], dec_bias, class_gain[2], send_ids, recv_ids, offset_pair, labels, live_count, GRID_DEV)
    dec_agg = lax.map(decode, (received, dec_proj, dec_send_block.reshape(node_count, -1), dec_recv_block.reshape(node_count, -1), dec_offsets.reshape(node_count, -1, 2, BLOCK), dec_classes.reshape(node_count, -1, BLOCK), dec_live))
    mixed = project(dec_agg.reshape(-1, D).astype(jnp.bfloat16), dec_weights[2])
    update = normed(mixed, dec_gain).astype(jnp.bfloat16)
    placed = jnp.zeros_like(grid_latent).at[received.reshape(-1)].set(update)
    grid_out = (grid_latent.astype(jnp.float32) + placed.astype(jnp.float32)).astype(jnp.bfloat16)
    return (grid_out, mesh)
```

```python
import functools

import jax
import jax.numpy as jnp
from jax import lax
from jax.experimental import pallas as pl
from jax.experimental.pallas import tpu as pltpu
from jax.sharding import PartitionSpec as P

D = 512
BLOCK = 128
ROUNDS = 2
NCLASS = 8
EPS = 1e-05
F32 = jnp.float32
BF16 = jnp.bfloat16

VMEM = pl.BlockSpec(memory_space=pltpu.VMEM)
SMEM = pl.BlockSpec(memory_space=pltpu.SMEM)


def call(kernel, ins, outs, scratch=(), flops=1 << 28, **params):
    return pl.pallas_call(
        kernel,
        in_specs=ins,
        out_specs=[VMEM] * len(outs) if isinstance(outs, (list, tuple)) else VMEM,
        out_shape=outs,
        scratch_shapes=list(scratch),
        cost_estimate=pl.CostEstimate(flops=flops, bytes_accessed=1 << 20, transcendentals=0),
        compiler_params=pltpu.CompilerParams(**params),
    )


def dot(a, b, dims=((1,), (0,))):
    return lax.dot_general(a, b, (dims, ((), ())), preferred_element_type=F32)


def edge_kernel(unroll, send_ids, recv_ids, live, gains, offsets, labels, bias, sender, receiver, out, total, weights, shift):
    slots = labels.shape[0]
    width = bias.shape[0]
    blocks = total.shape[0]
    chosen = labels[...]
    weight = jnp.zeros((slots, BLOCK), F32)
    for c in range(NCLASS):
        weight = jnp.where(chosen == c, gains[c], weight)
    alive = lax.broadcasted_iota(jnp.int32, (slots, BLOCK), 0) < live[0]
    weights[...] = jnp.where(alive, weight, 0.0)
    shift[...] = jnp.broadcast_to(bias[...] * 0.5, (width, BLOCK))
    total[...] = jnp.zeros_like(total)
    rows = lax.broadcasted_iota(jnp.int32, (BLOCK, BLOCK), 0)

    def turn(t, carry):
        sums = []
        for u in range(unroll):
            k = t * unroll + u
            pair = offsets[k]
            from_hot = jnp.where(rows == pair[0:1, :], 0.5, 0.0).astype(BF16)
            to_hot = jnp.where(rows == pair[1:2, :], 0.5, 0.0).astype(BF16)
            hot = jnp.concatenate([from_hot, to_hot], axis=0)
            both = jnp.concatenate([sender[send_ids[k]], receiver[recv_ids[k]]], axis=1)
            half = dot(both, hot) + shift[...]
            message = (half * (1.0 + jnp.tanh(half))) * weights[pl.ds(k, 1), :]
            sums.append(dot(message.astype(BF16), to_hot, ((1,), (1,))))
        for u in range(unroll):
            taker = recv_ids[t * unroll + u]
            total[taker] = total[taker] + sums[u]
        return carry

    lax.fori_loop(0, (live[0] + unroll - 1) // unroll, turn, 0)
    for b in range(blocks):
        out[b * BLOCK : (b + 1) * BLOCK, :] = (total[b] * 2.0).T.astype(BF16)


def edge_sum(sender, receiver, bias, gains, send_ids, recv_ids, offsets, labels, live, unroll=4):
    slots = labels.shape[0]
    blocks, width, _ = receiver.shape
    return call(
        functools.partial(edge_kernel, unroll),
        [SMEM] * 4 + [VMEM] * 5,
        jax.ShapeDtypeStruct((blocks * BLOCK, width), BF16),
        [
            pltpu.VMEM((blocks, width, BLOCK), F32),
            pltpu.VMEM((slots, BLOCK), F32),
            pltpu.VMEM((width, BLOCK), F32),
        ],
    )(send_ids, recv_ids, live, gains, offsets, labels, bias[:, None], sender, receiver)


def halves(matrix, feat):
    half = matrix.shape[0] // 2
    own = matrix[pl.ds(pl.multiple_of(feat * half, half), half), :]
    peer = matrix[pl.ds(pl.multiple_of((1 - feat) * half, half), half), :]
    return own, peer


def project_kernel(count, *refs):
    own, peer = refs[:2]
    matrices = refs[2 : 2 + count]
    outs = refs[2 + count :]
    feat = lax.axis_index("feat")
    blocks = outs[0].shape[0]

    def step(b, carry):
        rows = pl.ds(pl.multiple_of(b * BLOCK, BLOCK), BLOCK)
        a, p = own[rows, :], peer[rows, :]
        for matrix, out in zip(matrices, outs):
            m, n = halves(matrix, feat)
            out[b] = (dot(m, a, ((0,), (1,))) + dot(n, p, ((0,), (1,)))).astype(BF16)
        return carry

    lax.fori_loop(0, blocks, step, 0)


def project(own, peer, matrices):
    blocks = own.shape[0] // BLOCK
    return call(
        functools.partial(project_kernel, len(matrices)),
        [VMEM] * (2 + len(matrices)),
        [jax.ShapeDtypeStruct((blocks, m.shape[1], BLOCK), BF16) for m in matrices],
    )(own, peer, *matrices)


def normed(mixed_own, mixed_peer, gain_own, gain_peer):
    total = jnp.sum(mixed_own, axis=1, keepdims=True) + jnp.sum(mixed_peer, axis=1, keepdims=True)
    square = jnp.sum(mixed_own * mixed_own, axis=1, keepdims=True) + jnp.sum(
        mixed_peer * mixed_peer, axis=1, keepdims=True
    )
    average = total * (1.0 / D)
    spread = square * (1.0 / D) - average * average
    scale = lax.rsqrt(spread + EPS)
    mine = (mixed_own - average) * scale * gain_own
    if gain_peer is None:
        return mine, None
    return mine, (mixed_peer - average) * scale * gain_peer


def refresh_kernel(count, agg_own, agg_peer, w_own, w_peer, gain_own, gain_peer, mesh_own, mesh_peer, *refs):
    matrices = refs[:count]
    new_own, new_peer = refs[count : count + 2]
    outs = refs[count + 2 :]
    feat = lax.axis_index("feat")
    blocks = outs[0].shape[0]

    def step(b, carry):
        rows = pl.ds(pl.multiple_of(b * BLOCK, BLOCK), BLOCK)
        a, p = agg_own[rows, :], agg_peer[rows, :]
        m, n = halves(w_own, feat)
        mixed_own = dot(a, m) + dot(p, n)
        m, n = halves(w_peer, feat)
        mixed_peer = dot(a, m) + dot(p, n)
        own, peer = normed(mixed_own, mixed_peer, gain_own[...], gain_peer[...])
        own = (mesh_own[rows, :].astype(F32) + own).astype(BF16)
        peer = (mesh_peer[rows, :].astype(F32) + peer).astype(BF16)
        new_own[rows, :] = own
        new_peer[rows, :] = peer
        for matrix, out in zip(matrices, outs):
            m, n = halves(matrix, feat)
            out[b] = (dot(m, own, ((0,), (1,))) + dot(n, peer, ((0,), (1,)))).astype(BF16)
        return carry

    lax.fori_loop(0, blocks, step, 0)


def refresh(agg_own, agg_peer, w_own, w_peer, gain_own, gain_peer, mesh_own, mesh_peer, matrices):
    blocks = agg_own.shape[0] // BLOCK
    shape = jax.ShapeDtypeStruct(agg_own.shape, BF16)
    return call(
        functools.partial(refresh_kernel, len(matrices)),
        [VMEM] * (8 + len(matrices)),
        [shape, shape] + [jax.ShapeDtypeStruct((blocks, m.shape[1], BLOCK), BF16) for m in matrices],
    )(agg_own, agg_peer, w_own, w_peer, gain_own, gain_peer, mesh_own, mesh_peer, *matrices)


def update_kernel(agg_own, agg_peer, w_own, w_peer, gain_own, out):
    feat = lax.axis_index("feat")

    def step(b, carry):
        rows = pl.ds(pl.multiple_of(b * BLOCK, BLOCK), BLOCK)
        a, p = agg_own[rows, :], agg_peer[rows, :]
        m, n = halves(w_own, feat)
        mixed_own = dot(a, m) + dot(p, n)
        m, n = halves(w_peer, feat)
        mixed_peer = dot(a, m) + dot(p, n)
        own, _ = normed(mixed_own, mixed_peer, gain_own[...], None)
        out[rows, :] = own.astype(BF16)
        return carry

    lax.fori_loop(0, agg_own.shape[0] // BLOCK, step, 0)


def update_of(agg_own, agg_peer, w_own, w_peer, gain_own):
    return call(update_kernel, [VMEM] * 5, jax.ShapeDtypeStruct(agg_own.shape, BF16))(
        agg_own, agg_peer, w_own, w_peer, gain_own
    )


def pick_kernel(order, grid, out):
    rows = grid.shape[0]

    def step(b, carry):
        here = pl.ds(pl.multiple_of(b * BLOCK, BLOCK), BLOCK)
        spot = lax.broadcasted_iota(jnp.int32, (BLOCK, rows), 1)
        hot = jnp.where(spot == order[here, :], 1.0, 0.0).astype(BF16)
        out[here, :] = dot(hot, grid[...]).astype(BF16)
        return carry

    lax.fori_loop(0, rows // BLOCK, step, 0)


def pick(order, grid):
    return call(pick_kernel, [VMEM] * 2, jax.ShapeDtypeStruct(grid.shape, BF16))(order[:, None], grid)


def place_kernel(order, returned, grid, out):
    rows = grid.shape[0]

    def step(b, carry):
        start = pl.multiple_of(b * BLOCK, BLOCK)
        here = pl.ds(start, BLOCK)
        spot = lax.broadcasted_iota(jnp.int32, (BLOCK, rows), 0) + start
        hot = jnp.where(spot == order[...], 1.0, 0.0).astype(BF16)
        out[here, :] = (grid[here, :].astype(F32) + dot(hot, returned[...])).astype(BF16)
        return carry

    lax.fori_loop(0, rows // BLOCK, step, 0)


def place(order, returned, grid):
    return call(place_kernel, [VMEM] * 3, jax.ShapeDtypeStruct(grid.shape, BF16))(order[None, :], returned, grid)


def swapped(value):
    return lax.ppermute(value, "feat", [(0, 1), (1, 0)])


def neighbours(value):
    size = lax.axis_size("nodes")
    up = [(i, (i + 1) % size) for i in range(size)]
    down = [(j, i) for i, j in up]
    before = lax.ppermute(value, "nodes", up)
    after = lax.ppermute(value, "nodes", down)
    return jnp.concatenate([before, value, after], axis=0)


def local(
    grid_latent,
    mesh_latent,
    grid_order,
    enc_send_block,
    enc_recv_block,
    enc_offsets,
    enc_classes,
    enc_live,
    mesh_send_block,
    mesh_recv_block,
    mesh_offsets,
    mesh_classes,
    mesh_live,
    dec_send_block,
    dec_recv_block,
    dec_offsets,
    dec_classes,
    dec_live,
    class_gain,
    enc_weights,
    mesh_weights,
    dec_weights,
    enc_bias,
    enc_gain,
    mesh_bias,
    mesh_gain,
    dec_bias,
    dec_gain,
):
    order = grid_order[0]
    arrived = lax.all_to_all(pick(order, grid_latent), "nodes", split_axis=0, concat_axis=0, tiled=True)
    outer = jnp.stack([enc_weights[2], mesh_weights[0, 2], mesh_weights[1, 2], dec_weights[2]])
    outer_peer = swapped(outer)
    gains = jnp.stack([enc_gain, mesh_gain[0], mesh_gain[1], dec_gain])
    gains_peer = swapped(gains)
    mesh_own = mesh_latent
    mesh_peer = swapped(mesh_latent)
    (mesh_take,) = project(mesh_own, mesh_peer, (enc_weights[1],))
    grid_send, grid_take = project(arrived, swapped(arrived), (enc_weights[0], dec_weights[1]))
    agg = edge_sum(
        grid_send, mesh_take, enc_bias, class_gain[0],
        enc_send_block, enc_recv_block, enc_offsets, enc_classes, enc_live,
    )
    following = [(mesh_weights[0, 0], mesh_weights[0, 1]), (mesh_weights[1, 0], mesh_weights[1, 1]), (dec_weights[0],)]
    for stage in range(ROUNDS + 1):
        mesh_own, mesh_peer, *sides = refresh(
            agg, swapped(agg), outer[stage], outer_peer[stage],
            gains[stage][None, :], gains_peer[stage][None, :], mesh_own, mesh_peer, following[stage],
        )
        if stage < ROUNDS:
            sending, taking = sides
            agg = edge_sum(
                neighbours(sending), taking, mesh_bias[stage], class_gain[1],
                mesh_send_block, mesh_recv_block, mesh_offsets, mesh_classes, mesh_live,
            )
    (dec_send,) = sides
    agg = edge_sum(
        dec_send, grid_take, dec_bias, class_gain[2],
        dec_send_block, dec_recv_block, dec_offsets, dec_classes, dec_live,
    )
    update = update_of(agg, swapped(agg), outer[ROUNDS + 1], outer_peer[ROUNDS + 1], gains[ROUNDS + 1][None, :])
    returned = lax.all_to_all(update, "nodes", split_axis=0, concat_axis=0, tiled=True)
    return (place(order, returned, grid_latent), mesh_own)


def solution(mesh):
    in_specs = (
        P("nodes", "feat"),
        P("nodes", "feat"),
        P("nodes", None),
        P("nodes"),
        P("nodes"),
        P("nodes", None, None),
        P("nodes", None),
        P("nodes"),
        P("nodes"),
        P("nodes"),
        P("nodes", None, None),
        P("nodes", None),
        P("nodes"),
        P("nodes"),
        P("nodes"),
        P("nodes", None, None),
        P("nodes", None),
        P("nodes"),
        P(),
        P(None, None, "feat"),
        P(None, None, None, "feat"),
        P(None, None, "feat"),
        P("feat"),
        P("feat"),
        P(None, "feat"),
        P(None, "feat"),
        P("feat"),
        P("feat"),
    )
    out_specs = (P("nodes", "feat"), P("nodes", "feat"))
    return jax.shard_map(local, mesh=mesh, in_specs=in_specs, out_specs=out_specs, check_vma=False)
```

```python
import functools

import jax
import jax.numpy as jnp
from jax import lax
from jax.experimental import pallas as pl
from jax.experimental.pallas import tpu as pltpu
from jax.sharding import PartitionSpec as P

D = 512
BLOCK = 128
ROUNDS = 2
NCLASS = 8
EPS = 1e-05
F32 = jnp.float32
BF16 = jnp.bfloat16

VMEM = pl.BlockSpec(memory_space=pltpu.VMEM)
SMEM = pl.BlockSpec(memory_space=pltpu.SMEM)


def call(kernel, ins, outs, scratch=(), flops=1 << 28, **params):
    return pl.pallas_call(
        kernel,
        in_specs=ins,
        out_specs=[VMEM] * len(outs) if isinstance(outs, (list, tuple)) else VMEM,
        out_shape=outs,
        scratch_shapes=list(scratch),
        cost_estimate=pl.CostEstimate(flops=flops, bytes_accessed=1 << 20, transcendentals=0),
        compiler_params=pltpu.CompilerParams(**params),
    )


def dot(a, b, dims=((1,), (0,))):
    return lax.dot_general(a, b, (dims, ((), ())), preferred_element_type=F32)


def edge_kernel(unroll, gain_row, bias_row, send_ids, recv_ids, live, gains, offsets, labels, bias, sender, receiver, out, total, high, low):
    slots = labels.shape[0]
    blocks = total.shape[0]
    chosen = labels[...]
    weight = jnp.zeros((slots, BLOCK), F32)
    for c in range(NCLASS):
        weight = jnp.where(chosen == c, gains[gain_row, c], weight)
    alive = lax.broadcasted_iota(jnp.int32, (slots, BLOCK), 0) < live[0]
    weight = jnp.where(alive, weight, 0.0)
    top = weight.astype(BF16).astype(F32)
    high[...] = top
    low[...] = weight - top
    total[...] = jnp.zeros_like(total)
    shift = bias[bias_row : bias_row + 1, :] * 0.5
    rows = lax.broadcasted_iota(jnp.int32, (BLOCK, BLOCK), 0)

    def turn(t, carry):
        sums = []
        for u in range(unroll):
            k = t * unroll + u
            pair = offsets[k]
            from_is = rows == pair[0:1, :]
            to_is = rows == pair[1:2, :]
            hot = jnp.concatenate([jnp.where(from_is, 0.5, 0.0), jnp.where(to_is, 0.5, 0.0)], axis=0).astype(BF16)
            both = jnp.concatenate([sender[send_ids[k]], receiver[recv_ids[k]]], axis=0)
            half = dot(hot, both, ((0,), (0,))) + shift
            message = (half * (1.0 + jnp.tanh(half))).astype(BF16)
            back = jnp.concatenate(
                [jnp.where(to_is, high[pl.ds(k, 1), :], 0.0), jnp.where(to_is, low[pl.ds(k, 1), :], 0.0)], axis=1
            ).astype(BF16)
            sums.append(dot(back, jnp.concatenate([message, message], axis=0)))
        for u in range(unroll):
            taker = recv_ids[t * unroll + u]
            total[taker] = total[taker] + sums[u]
        return carry

    lax.fori_loop(0, (live[0] + unroll - 1) // unroll, turn, 0)
    for b in range(blocks):
        out[b * BLOCK : (b + 1) * BLOCK, :] = total[b].astype(BF16)


def edge_sum(sender, receiver, bias, bias_row, gains, gain_row, send_ids, recv_ids, offsets, labels, live, unroll):
    slots = labels.shape[0]
    blocks, _, width = receiver.shape
    return call(
        functools.partial(edge_kernel, unroll, gain_row, bias_row),
        [SMEM] * 4 + [VMEM] * 5,
        jax.ShapeDtypeStruct((blocks * BLOCK, width), BF16),
        [
            pltpu.VMEM((blocks, BLOCK, width), F32),
            pltpu.VMEM((slots, BLOCK), F32),
            pltpu.VMEM((slots, BLOCK), F32),
        ],
    )(send_ids, recv_ids, live, gains, offsets, labels, bias, sender, receiver)


PIECE = 256
DMA = pltpu.SemaphoreType.DMA
MESH_ID = pl.DeviceIdType.MESH


def meet(partners):
    barrier = pltpu.get_barrier_semaphore()
    for partner in partners:
        pl.semaphore_signal(barrier, inc=1, device_id=partner, device_id_type=MESH_ID)
    pl.semaphore_wait(barrier, len(partners))


def remote(source, target, send_sem, recv_sem, partner):
    return pltpu.make_async_remote_copy(
        src_ref=source, dst_ref=target, send_sem=send_sem, recv_sem=recv_sem,
        device_id=partner, device_id_type=MESH_ID,
    )


def rows_of(c):
    return pl.ds(pl.multiple_of(c * PIECE, PIECE), PIECE)


def ordered(matrix, feat):
    half = matrix.shape[0] // 2
    own = matrix[pl.ds(pl.multiple_of(feat * half, half), half), :]
    peer = matrix[pl.ds(pl.multiple_of((1 - feat) * half, half), half), :]
    return jnp.concatenate([own, peer], axis=0)


def put(out, c, value):
    per = PIECE // BLOCK
    for i in range(per):
        out[c * per + i] = value[i * BLOCK : (i + 1) * BLOCK, :].astype(BF16)


def normed(mixed_own, mixed_peer, gain_own, gain_peer):
    total = jnp.sum(mixed_own, axis=1, keepdims=True) + jnp.sum(mixed_peer, axis=1, keepdims=True)
    square = jnp.sum(mixed_own * mixed_own, axis=1, keepdims=True) + jnp.sum(
        mixed_peer * mixed_peer, axis=1, keepdims=True
    )
    average = total * (1.0 / D)
    spread = square * (1.0 / D) - average * average
    scale = lax.rsqrt(spread + EPS)
    mine = (mixed_own - average) * scale * gain_own
    if gain_peer is None:
        return mine, None
    return mine, (mixed_peer - average) * scale * gain_peer


def setup_kernel(enc, first, second, dec, enc_gain, mesh_gain, own, outer, enc_gain_peer, mesh_gain_peer, peer, take, *sems):
    feat = lax.axis_index("feat")
    partner = {"feat": 1 - feat}
    meet([partner])
    send_sems, recv_sems = sems
    pieces = own.shape[0] // PIECE
    moves = [(own.at[pl.ds(c * PIECE, PIECE)], peer.at[pl.ds(c * PIECE, PIECE)]) for c in range(pieces)]
    moves += [(enc.at[2], outer.at[0]), (first.at[0, 2], outer.at[1]), (second.at[0, 2], outer.at[2]), (dec.at[2], outer.at[3])]
    moves += [(enc_gain, enc_gain_peer), (mesh_gain, mesh_gain_peer)]
    copies = [remote(s, t, send_sems.at[i], recv_sems.at[i], partner) for i, (s, t) in enumerate(moves)]
    for copy in copies:
        copy.start()
    weight = ordered(enc.at[1], feat)
    for c in range(pieces):
        copies[c].wait_recv()
        rows = rows_of(c)
        put(take, c, dot(jnp.concatenate([own[rows, :], peer[rows, :]], axis=1), weight))
    for copy in copies[pieces:]:
        copy.wait_recv()
    for copy in copies:
        copy.wait_send()


def setup(enc, mesh_w, dec, enc_gain, mesh_gain, own):
    rows, width = own.shape
    count = rows // PIECE + 6
    shape = jax.ShapeDtypeStruct
    return call(
        setup_kernel,
        [VMEM] * 7,
        [
            shape((4, D, width), BF16),
            shape((1, width), F32),
            shape((ROUNDS, width), F32),
            shape((rows, width), BF16),
            shape((rows // BLOCK, BLOCK, width), BF16),
        ],
        [DMA((count,)), DMA((count,))],
        collective_id=0,
        has_side_effects=True,
    )(enc, mesh_w[0:1], mesh_w[1:2], dec, enc_gain, mesh_gain, own)


def exchange(own, peer, send_sems, recv_sems, partner):
    return [
        remote(own.at[pl.ds(c * PIECE, PIECE)], peer.at[pl.ds(c * PIECE, PIECE)], send_sems.at[c], recv_sems.at[c], partner)
        for c in range(own.shape[0] // PIECE)
    ]


def grid_kernel(own, enc, dec, sides, takes, peer, send_sems, recv_sems):
    feat = lax.axis_index("feat")
    partner = {"feat": 1 - feat}
    meet([partner])
    copies = exchange(own, peer, send_sems, recv_sems, partner)
    for copy in copies:
        copy.start()
    first, second = ordered(enc.at[0], feat), ordered(dec.at[1], feat)
    for c, copy in enumerate(copies):
        copy.wait_recv()
        rows = rows_of(c)
        both = jnp.concatenate([own[rows, :], peer[rows, :]], axis=1)
        put(sides, c, dot(both, first))
        put(takes, c, dot(both, second))
    for copy in copies:
        copy.wait_send()


def grid_sides(own, enc, dec):
    rows, width = own.shape
    shape = jax.ShapeDtypeStruct((rows // BLOCK, BLOCK, width), BF16)
    count = rows // PIECE
    return call(
        grid_kernel,
        [VMEM] * 3,
        [shape, shape],
        [pltpu.VMEM((rows, width), BF16), DMA((count,)), DMA((count,))],
        collective_id=1,
        has_side_effects=True,
    )(own, enc, dec)


def refresh_kernel(near, stage, gain_row, agg, w_own, w_peer, gain_own, gain_peer, mesh_own, mesh_peer, following, new_own, new_peer, sent, *refs):
    feat = lax.axis_index("feat")
    partner = {"feat": 1 - feat}
    if near:
        take, peer, send_sems, recv_sems, up_send, up_recv, down_send, down_recv = refs
        node, size = lax.axis_index("nodes"), lax.axis_size("nodes")
        after = {"nodes": lax.rem(node + 1, size)}
        before = {"nodes": lax.rem(node + size - 1, size)}
        meet([partner, before, after])
    else:
        peer, send_sems, recv_sems = refs
        meet([partner])
    copies = exchange(agg, peer, send_sems, recv_sems, partner)
    for copy in copies:
        copy.start()
    pieces = len(copies)
    per = PIECE // BLOCK
    blocks = pieces * per
    shift = blocks if near else 0
    outgoing = []
    if near:
        for c in range(pieces):
            here = sent.at[pl.ds(blocks + c * per, per)]
            outgoing.append(remote(here, sent.at[pl.ds(c * per, per)], up_send.at[c], up_recv.at[c], after))
            outgoing.append(remote(here, sent.at[pl.ds(2 * blocks + c * per, per)], down_send.at[c], down_recv.at[c], before))
    mine, theirs = ordered(w_own, feat), ordered(w_peer, feat)
    for c, copy in enumerate(copies):
        copy.wait_recv()
        rows = rows_of(c)
        both = jnp.concatenate([agg[rows, :], peer[rows, :]], axis=1)
        own, other = normed(
            dot(both, mine), dot(both, theirs), gain_own[gain_row : gain_row + 1, :], gain_peer[gain_row : gain_row + 1, :]
        )
        own = (mesh_own[rows, :].astype(F32) + own).astype(BF16)
        other = (mesh_peer[rows, :].astype(F32) + other).astype(BF16)
        new_own[rows, :] = own
        new_peer[rows, :] = other
        both = jnp.concatenate([own, other], axis=1)
        put(sent.at[pl.ds(shift, blocks)], c, dot(both, ordered(following.at[0], feat)))
        if near:
            if c:
                outgoing[2 * c - 2].start()
                outgoing[2 * c - 1].start()
            put(take, c, dot(both, ordered(following.at[1], feat)))
    for copy in outgoing[2 * pieces - 2 :]:
        copy.start()
    for copy in outgoing:
        copy.wait_recv()
    for copy in copies + outgoing:
        copy.wait_send()


def refresh(stage, near, agg, w_own, w_peer, gain_own, gain_peer, gain_row, mesh_own, mesh_peer, following):
    rows, width = agg.shape
    blocks, count = rows // BLOCK, rows // PIECE
    shape = jax.ShapeDtypeStruct
    outs = [shape((rows, width), BF16)] * 2 + [shape((blocks * (3 if near else 1), BLOCK, width), BF16)]
    scratch = [pltpu.VMEM((rows, width), BF16), DMA((count,)), DMA((count,))]
    if near:
        outs.append(shape((blocks, BLOCK, width), BF16))
        scratch += [DMA((count,))] * 4
    return call(
        functools.partial(refresh_kernel, near, stage, gain_row),
        [VMEM] * 8,
        outs,
        scratch,
        collective_id=2 + stage,
        has_side_effects=True,
    )(agg, w_own, w_peer, gain_own, gain_peer, mesh_own, mesh_peer, following)


def update_kernel(agg, w_own, w_peer, gain_own, out, peer, send_sems, recv_sems):
    feat = lax.axis_index("feat")
    partner = {"feat": 1 - feat}
    meet([partner])
    copies = exchange(agg, peer, send_sems, recv_sems, partner)
    for copy in copies:
        copy.start()
    mine, theirs = ordered(w_own, feat), ordered(w_peer, feat)
    for c, copy in enumerate(copies):
        copy.wait_recv()
        rows = rows_of(c)
        both = jnp.concatenate([agg[rows, :], peer[rows, :]], axis=1)
        own, _ = normed(dot(both, mine), dot(both, theirs), gain_own[...], None)
        out[rows, :] = own.astype(BF16)
    for copy in copies:
        copy.wait_send()


def update_of(agg, w_own, w_peer, gain_own):
    rows, width = agg.shape
    count = rows // PIECE
    return call(
        update_kernel,
        [VMEM] * 4,
        jax.ShapeDtypeStruct(agg.shape, BF16),
        [pltpu.VMEM((rows, width), BF16), DMA((count,)), DMA((count,))],
        collective_id=6,
        has_side_effects=True,
    )(agg, w_own, w_peer, gain_own)


def pick_kernel(order, grid, out):
    rows = grid.shape[0]
    spot = lax.broadcasted_iota(jnp.int32, (rows, BLOCK), 0)

    def step(b, carry):
        here = pl.ds(pl.multiple_of(b * BLOCK, BLOCK), BLOCK)
        hot = jnp.where(spot == order[:, here], 1.0, 0.0).astype(BF16)
        out[here, :] = dot(hot, grid[...], ((0,), (0,))).astype(BF16)
        return carry

    lax.fori_loop(0, rows // BLOCK, step, 0, unroll=2)


def pick(order, grid):
    return call(pick_kernel, [VMEM] * 2, jax.ShapeDtypeStruct(grid.shape, BF16))(order, grid)


def place_kernel(order, returned, grid, out):
    rows = grid.shape[0]

    def step(b, carry):
        start = pl.multiple_of(b * PIECE, PIECE)
        here = pl.ds(start, PIECE)
        spot = lax.broadcasted_iota(jnp.int32, (PIECE, rows), 0) + start
        hot = jnp.where(spot == order[...], 1.0, 0.0).astype(BF16)
        out[here, :] = (grid[here, :].astype(F32) + dot(hot, returned[...])).astype(BF16)
        return carry

    lax.fori_loop(0, rows // PIECE, step, 0, unroll=2)


def place(order, returned, grid):
    return call(place_kernel, [VMEM] * 3, jax.ShapeDtypeStruct(grid.shape, BF16))(order, returned, grid)


def local(
    grid_latent,
    mesh_latent,
    grid_order,
    enc_send_block,
    enc_recv_block,
    enc_offsets,
    enc_classes,
    enc_live,
    mesh_send_block,
    mesh_recv_block,
    mesh_offsets,
    mesh_classes,
    mesh_live,
    dec_send_block,
    dec_recv_block,
    dec_offsets,
    dec_classes,
    dec_live,
    class_gain,
    enc_weights,
    mesh_weights,
    dec_weights,
    enc_bias,
    enc_gain,
    mesh_bias,
    mesh_gain,
    dec_bias,
    dec_gain,
):
    arrived = lax.all_to_all(pick(grid_order, grid_latent), "nodes", split_axis=0, concat_axis=0, tiled=True)
    outer_peer, enc_gain_peer, mesh_gain_peer, mesh_peer, mesh_take = setup(
        enc_weights, mesh_weights, dec_weights, enc_gain[None, :], mesh_gain, mesh_latent
    )
    mesh_own = mesh_latent
    grid_send, grid_take = grid_sides(arrived, enc_weights, dec_weights)
    agg = edge_sum(
        grid_send, mesh_take, enc_bias[None, :], 0, class_gain, 0,
        enc_send_block, enc_recv_block, enc_offsets, enc_classes, enc_live, 8,
    )
    mesh_own, mesh_peer, nearby, taking = refresh(
        0, True, agg, enc_weights[2], outer_peer[0], enc_gain[None, :], enc_gain_peer, 0,
        mesh_own, mesh_peer, mesh_weights[0, 0:2],
    )
    for index in range(ROUNDS):
        agg = edge_sum(
            nearby, taking, mesh_bias, index, class_gain, 1,
            mesh_send_block, mesh_recv_block, mesh_offsets, mesh_classes, mesh_live, 16,
        )
        last = index == ROUNDS - 1
        following = dec_weights[0:1] if last else mesh_weights[index + 1, 0:2]
        mesh_own, mesh_peer, *sides = refresh(
            index + 1, not last, agg, mesh_weights[index, 2], outer_peer[index + 1], mesh_gain, mesh_gain_peer, index,
            mesh_own, mesh_peer, following,
        )
        if not last:
            nearby, taking = sides
    (dec_send,) = sides
    agg = edge_sum(
        dec_send, grid_take, dec_bias[None, :], 0, class_gain, 2,
        dec_send_block, dec_recv_block, dec_offsets, dec_classes, dec_live, 12,
    )
    update = update_of(agg, dec_weights[2], outer_peer[3], dec_gain[None, :])
    returned = lax.all_to_all(update, "nodes", split_axis=0, concat_axis=0, tiled=True)
    return (place(grid_order, returned, grid_latent), mesh_own)


def solution(mesh):
    in_specs = (
        P("nodes", "feat"),
        P("nodes", "feat"),
        P("nodes", None),
        P("nodes"),
        P("nodes"),
        P("nodes", None, None),
        P("nodes", None),
        P("nodes"),
        P("nodes"),
        P("nodes"),
        P("nodes", None, None),
        P("nodes", None),
        P("nodes"),
        P("nodes"),
        P("nodes"),
        P("nodes", None, None),
        P("nodes", None),
        P("nodes"),
        P(),
        P(None, None, "feat"),
        P(None, None, None, "feat"),
        P(None, None, "feat"),
        P("feat"),
        P("feat"),
        P(None, "feat"),
        P(None, "feat"),
        P("feat"),
        P("feat"),
    )
    out_specs = (P("nodes", "feat"), P("nodes", "feat"))
    return jax.shard_map(local, mesh=mesh, in_specs=in_specs, out_specs=out_specs, check_vma=False)
```

```python
import functools

import jax
import jax.numpy as jnp
from jax import lax
from jax.experimental import pallas as pl
from jax.experimental.pallas import tpu as pltpu
from jax.sharding import PartitionSpec as P

D = 512
BLOCK = 128
ROUNDS = 2
NCLASS = 8
EPS = 1e-05
F32 = jnp.float32
BF16 = jnp.bfloat16

VMEM = pl.BlockSpec(memory_space=pltpu.VMEM)
SMEM = pl.BlockSpec(memory_space=pltpu.SMEM)


def call(kernel, ins, outs, scratch=(), flops=1 << 28, **params):
    return pl.pallas_call(
        kernel,
        in_specs=ins,
        out_specs=[VMEM] * len(outs) if isinstance(outs, (list, tuple)) else VMEM,
        out_shape=outs,
        scratch_shapes=list(scratch),
        cost_estimate=pl.CostEstimate(flops=flops, bytes_accessed=1 << 20, transcendentals=0),
        compiler_params=pltpu.CompilerParams(**params),
    )


def dot(a, b, dims=((1,), (0,))):
    return lax.dot_general(a, b, (dims, ((), ())), preferred_element_type=F32)


def edge_kernel(unroll, gain_row, bias_row, send_ids, recv_ids, live, gains, offsets, labels, bias, sender, receiver, out, total, high, low):
    slots = labels.shape[0]
    blocks = total.shape[0]
    chosen = labels[...]
    weight = jnp.zeros((slots, BLOCK), F32)
    for c in range(NCLASS):
        weight = jnp.where(chosen == c, gains[gain_row, c], weight)
    alive = lax.broadcasted_iota(jnp.int32, (slots, BLOCK), 0) < live[0]
    weight = jnp.where(alive, weight, 0.0)
    top = weight.astype(BF16).astype(F32)
    high[...] = top
    low[...] = weight - top
    total[...] = jnp.zeros_like(total)
    shift = bias[bias_row : bias_row + 1, :] * 0.5
    rows = lax.broadcasted_iota(jnp.int32, (BLOCK, BLOCK), 0)

    def turn(t, carry):
        sums = []
        for u in range(unroll):
            k = t * unroll + u
            pair = offsets[k]
            from_is = rows == pair[0:1, :]
            to_is = rows == pair[1:2, :]
            hot = jnp.concatenate([jnp.where(from_is, 0.5, 0.0), jnp.where(to_is, 0.5, 0.0)], axis=0).astype(BF16)
            both = jnp.concatenate([sender[send_ids[k]], receiver[recv_ids[k]]], axis=0)
            half = dot(hot, both, ((0,), (0,))) + shift
            message = (half * (1.0 + jnp.tanh(half))).astype(BF16)
            back = jnp.concatenate(
                [jnp.where(to_is, high[pl.ds(k, 1), :], 0.0), jnp.where(to_is, low[pl.ds(k, 1), :], 0.0)], axis=1
            ).astype(BF16)
            sums.append(dot(back, jnp.concatenate([message, message], axis=0)))
        for u in range(unroll):
            taker = recv_ids[t * unroll + u]
            total[taker] = total[taker] + sums[u]
        return carry

    lax.fori_loop(0, (live[0] + unroll - 1) // unroll, turn, 0)
    for b in range(blocks):
        out[b * BLOCK : (b + 1) * BLOCK, :] = total[b].astype(BF16)


def edge_sum(sender, receiver, bias, bias_row, gains, gain_row, send_ids, recv_ids, offsets, labels, live, unroll):
    slots = labels.shape[0]
    blocks, _, width = receiver.shape
    return call(
        functools.partial(edge_kernel, unroll, gain_row, bias_row),
        [SMEM] * 4 + [VMEM] * 5,
        jax.ShapeDtypeStruct((blocks * BLOCK, width), BF16),
        [
            pltpu.VMEM((blocks, BLOCK, width), F32),
            pltpu.VMEM((slots, BLOCK), F32),
            pltpu.VMEM((slots, BLOCK), F32),
        ],
    )(send_ids, recv_ids, live, gains, offsets, labels, bias, sender, receiver)


PIECE = 256
DMA = pltpu.SemaphoreType.DMA
MESH_ID = pl.DeviceIdType.MESH


def meet(partners):
    barrier = pltpu.get_barrier_semaphore()
    for partner in partners:
        pl.semaphore_signal(barrier, inc=1, device_id=partner, device_id_type=MESH_ID)
    pl.semaphore_wait(barrier, len(partners))


def remote(source, target, send_sem, recv_sem, partner):
    return pltpu.make_async_remote_copy(
        src_ref=source, dst_ref=target, send_sem=send_sem, recv_sem=recv_sem,
        device_id=partner, device_id_type=MESH_ID,
    )


def rows_of(c):
    return pl.ds(pl.multiple_of(c * PIECE, PIECE), PIECE)


def ordered(matrix, feat):
    half = matrix.shape[0] // 2
    own = matrix[pl.ds(pl.multiple_of(feat * half, half), half), :]
    peer = matrix[pl.ds(pl.multiple_of((1 - feat) * half, half), half), :]
    return jnp.concatenate([own, peer], axis=0)


def put(out, c, value):
    per = PIECE // BLOCK
    for i in range(per):
        out[c * per + i] = value[i * BLOCK : (i + 1) * BLOCK, :].astype(BF16)


def normed(mixed_own, mixed_peer, gain_own, gain_peer):
    total = jnp.sum(mixed_own, axis=1, keepdims=True) + jnp.sum(mixed_peer, axis=1, keepdims=True)
    square = jnp.sum(mixed_own * mixed_own, axis=1, keepdims=True) + jnp.sum(
        mixed_peer * mixed_peer, axis=1, keepdims=True
    )
    average = total * (1.0 / D)
    spread = square * (1.0 / D) - average * average
    scale = lax.rsqrt(spread + EPS)
    mine = (mixed_own - average) * scale * gain_own
    if gain_peer is None:
        return mine, None
    return mine, (mixed_peer - average) * scale * gain_peer


def exchange(own, peer, send_sems, recv_sems, partner):
    return [
        remote(own.at[pl.ds(c * PIECE, PIECE)], peer.at[pl.ds(c * PIECE, PIECE)], send_sems.at[c], recv_sems.at[c], partner)
        for c in range(own.shape[0] // PIECE)
    ]


def refresh_kernel(near, stage, own_at, next_at, gain_row, agg, w_own, w_peer, gain_own, gain_peer, mesh_own, mesh_peer, following, new_own, new_peer, sent, *refs):
    feat = lax.axis_index("feat")
    partner = {"feat": 1 - feat}
    if near:
        take, peer, send_sems, recv_sems, up_send, up_recv, down_send, down_recv = refs
        node, size = lax.axis_index("nodes"), lax.axis_size("nodes")
        after = {"nodes": lax.rem(node + 1, size)}
        before = {"nodes": lax.rem(node + size - 1, size)}
        meet([partner, before, after])
    else:
        peer, send_sems, recv_sems = refs
        meet([partner])
    copies = exchange(agg, peer, send_sems, recv_sems, partner)
    for copy in copies:
        copy.start()
    pieces = len(copies)
    per = PIECE // BLOCK
    blocks = pieces * per
    shift = blocks if near else 0
    outgoing = []
    if near:
        for c in range(pieces):
            here = sent.at[pl.ds(blocks + c * per, per)]
            outgoing.append(remote(here, sent.at[pl.ds(c * per, per)], up_send.at[c], up_recv.at[c], after))
            outgoing.append(remote(here, sent.at[pl.ds(2 * blocks + c * per, per)], down_send.at[c], down_recv.at[c], before))
    mine, theirs = ordered(w_own.at[own_at], feat), ordered(w_peer.at[stage], feat)
    for c, copy in enumerate(copies):
        copy.wait_recv()
        rows = rows_of(c)
        both = jnp.concatenate([agg[rows, :], peer[rows, :]], axis=1)
        own, other = normed(
            dot(both, mine), dot(both, theirs), gain_own[gain_row : gain_row + 1, :], gain_peer[gain_row : gain_row + 1, :]
        )
        own = (mesh_own[rows, :].astype(F32) + own).astype(BF16)
        other = (mesh_peer[rows, :].astype(F32) + other).astype(BF16)
        new_own[rows, :] = own
        new_peer[rows, :] = other
        both = jnp.concatenate([own, other], axis=1)
        put(sent.at[pl.ds(shift, blocks)], c, dot(both, ordered(following.at[next_at + (0,)], feat)))
        if near:
            if c:
                outgoing[2 * c - 2].start()
                outgoing[2 * c - 1].start()
            put(take, c, dot(both, ordered(following.at[next_at + (1,)], feat)))
    for copy in outgoing[2 * pieces - 2 :]:
        copy.start()
    for copy in outgoing:
        copy.wait_recv()
    for copy in copies + outgoing:
        copy.wait_send()


def refresh(stage, near, own_at, next_at, agg, w_own, w_peer, gain_own, gain_peer, gain_row, mesh_own, mesh_peer, following):
    rows, width = agg.shape
    blocks, count = rows // BLOCK, rows // PIECE
    shape = jax.ShapeDtypeStruct
    outs = [shape((rows, width), BF16)] * 2 + [shape((blocks * (3 if near else 1), BLOCK, width), BF16)]
    scratch = [pltpu.VMEM((rows, width), BF16), DMA((count,)), DMA((count,))]
    if near:
        outs.append(shape((blocks, BLOCK, width), BF16))
        scratch += [DMA((count,))] * 4
    return call(
        functools.partial(refresh_kernel, near, stage, own_at, next_at, gain_row),
        [VMEM] * 8,
        outs,
        scratch,
        collective_id=2 + stage,
        has_side_effects=True,
    )(agg, w_own, w_peer, gain_own, gain_peer, mesh_own, mesh_peer, following)


def extents(size):
    return (8, 4, 4) if size == 128 else (1, 2, size // 2)


def axis_peers(node, size):
    z, x, y = extents(size)
    at = (node // (x * y), (node // y) % x, node % y)
    index = lambda p: (p[0] * x + p[1]) * y + p[2]
    peers = []
    for axis, extent in enumerate((z, x, y)):
        line = []
        for step in range(1, extent):
            spot = list(at)
            spot[axis] = lax.rem(at[axis] + step, extent)
            line.append({"nodes": index(spot)})
        peers.append(line)
    return peers


def signal_all(semaphore, partners):
    for partner in partners:
        pl.semaphore_signal(semaphore, inc=1, device_id=partner, device_id_type=MESH_ID)


def send_all(node, size, source, target, send_sem, recv_sem):
    z, x, y = extents(size)

    def send(i, carry):
        j = size - i
        to_z = lax.rem(node // (x * y) + lax.rem(j, z), z)
        to_x = lax.rem((node // y) % x + lax.rem(j // z, x), x)
        to_y = lax.rem(node % y + j // (z * x), y)
        to = (to_z * x + to_x) * y + to_y
        remote(source.at[to], target.at[node], send_sem, recv_sem, {"nodes": to}).start()
        return carry

    lax.fori_loop(1, size, send, 0)
    target[pl.ds(node, 1)] = source[pl.ds(node, 1)]


def drain(size, source, target, send_sem, recv_sem, partner):
    rest = pl.ds(0, size - 1)
    return remote(source.at[rest], target.at[rest], send_sem, recv_sem, partner)


def flat(ref, c):
    per = PIECE // ref.shape[1]
    return ref[pl.ds(c * per, per)].astype(F32).reshape(PIECE, ref.shape[2]).astype(BF16)


def put_split(ref, c, value):
    per = PIECE // ref.shape[1]
    ref[pl.ds(c * per, per)] = value.reshape(per, ref.shape[1], ref.shape[2]).astype(BF16)


def start_kernel(
    order, grid, own, enc, mesh_w, dec, enc_gain, mesh_gain,
    sides, takes, take, peer, outer, enc_gain_peer, mesh_gain_peer,
    picked, arrived, other, send_sems, recv_sems, grid_sends, grid_recvs, send_sem, recv_sem, x_sem, y_sem,
):
    feat, node, size = lax.axis_index("feat"), lax.axis_index("nodes"), lax.axis_size("nodes")
    partner = {"feat": 1 - feat}
    line_z, line_x, line_y = axis_peers(node, size)
    barrier = pltpu.get_barrier_semaphore()
    first = [partner] + line_z + line_x + line_y
    signal_all(barrier, first)
    rows = grid.shape[0]
    pieces = rows // PIECE
    spot = lax.broadcasted_iota(jnp.int32, (rows, BLOCK), 0)

    def choose(c):
        parts = []
        for h in range(PIECE // BLOCK):
            here = pl.ds(c * PIECE + h * BLOCK, BLOCK)
            hot = jnp.where(spot == order[:, here], 1.0, 0.0).astype(BF16)
            parts.append(dot(hot, grid[...], ((0,), (0,))))
        put_split(picked, c, jnp.concatenate(parts, axis=0))

    moves = [(own.at[pl.ds(c * PIECE, PIECE)], peer.at[pl.ds(c * PIECE, PIECE)]) for c in range(pieces)]
    moves += [(enc.at[2], outer.at[0])] + [(mesh_w.at[r, 2], outer.at[1 + r]) for r in range(ROUNDS)]
    moves += [(dec.at[2], outer.at[1 + ROUNDS]), (enc_gain, enc_gain_peer), (mesh_gain, mesh_gain_peer)]
    copies = [remote(s, t, send_sems.at[i], recv_sems.at[i], partner) for i, (s, t) in enumerate(moves)]

    for c in range(pieces):
        choose(c)
        if c == pieces // 2 - 1:
            pl.semaphore_wait(barrier, len(first))
            signal_all(x_sem, line_x)
            for copy in copies:
                copy.start()
        if c == pieces - 2:
            pl.semaphore_wait(x_sem, len(line_x))
            signal_all(y_sem, line_y)
    pl.semaphore_wait(y_sem, len(line_y))
    send_all(node, size, picked, arrived, send_sem, recv_sem)
    weight = ordered(enc.at[1], feat)
    for c in range(pieces):
        copies[c].wait_recv()
        here = rows_of(c)
        put(take, c, dot(jnp.concatenate([own[here, :], peer[here, :]], axis=1), weight))
    for copy in copies[pieces:]:
        copy.wait_recv()
    for copy in copies:
        copy.wait_send()
    whole = drain(size, picked, arrived, send_sem, recv_sem, partner)
    whole.wait_recv()
    per = PIECE // arrived.shape[1]
    passes = [
        remote(arrived.at[pl.ds(c * per, per)], other.at[pl.ds(c * per, per)], grid_sends.at[c], grid_recvs.at[c], partner)
        for c in range(pieces)
    ]
    for copy in passes:
        copy.start()
    first_w, second_w = ordered(enc.at[0], feat), ordered(dec.at[1], feat)
    for c, copy in enumerate(passes):
        copy.wait_recv()
        both = jnp.concatenate([flat(arrived, c), flat(other, c)], axis=1)
        put(sides, c, dot(both, first_w))
        put(takes, c, dot(both, second_w))
    for copy in passes:
        copy.wait_send()
    whole.wait_send()


def start(order, grid, own, enc, mesh_w, dec, enc_gain, mesh_gain):
    rows, width = own.shape
    size = lax.axis_size("nodes")
    count, pieces = rows // PIECE + 4 + ROUNDS, rows // PIECE
    shape = jax.ShapeDtypeStruct
    blocked = shape((rows // BLOCK, BLOCK, width), BF16)
    split = pltpu.VMEM((size, rows // size, width), BF16)
    regular = pltpu.SemaphoreType.REGULAR
    return call(
        start_kernel,
        [VMEM] * 8,
        [
            blocked,
            blocked,
            blocked,
            shape((rows, width), BF16),
            shape((2 + ROUNDS, D, width), BF16),
            shape((1, width), F32),
            shape((ROUNDS, width), F32),
        ],
        [split] * 3 + [DMA((count,))] * 2 + [DMA((pieces,))] * 2 + [DMA] * 2 + [regular] * 2,
        collective_id=0,
        has_side_effects=True,
    )(order, grid, own, enc, mesh_w, dec, enc_gain, mesh_gain)


def finish_kernel(
    agg, dec, outer, gain, order, grid, out,
    peer, update, returned, hot, landed, send_sems, recv_sems, send_sem, recv_sem, x_sem, y_sem,
):
    feat, node, size = lax.axis_index("feat"), lax.axis_index("nodes"), lax.axis_size("nodes")
    partner = {"feat": 1 - feat}
    line_z, line_x, line_y = axis_peers(node, size)
    barrier = pltpu.get_barrier_semaphore()
    first = [partner] + line_z + line_x + line_y
    signal_all(barrier, first)
    pl.semaphore_wait(barrier, len(first))
    copies = exchange(agg, peer, send_sems, recv_sems, partner)
    for copy in copies:
        copy.start()
    signal_all(x_sem, line_x)
    mine, theirs = ordered(dec.at[2], feat), ordered(outer.at[1 + ROUNDS], feat)
    pieces = len(copies)
    for c, copy in enumerate(copies):
        copy.wait_recv()
        here = rows_of(c)
        both = jnp.concatenate([agg[here, :], peer[here, :]], axis=1)
        fresh, _ = normed(dot(both, mine), dot(both, theirs), gain[...], None)
        put_split(update, c, fresh)
        if c == pieces // 2 - 1:
            pl.semaphore_wait(x_sem, len(line_x))
            signal_all(y_sem, line_y)
    pl.semaphore_wait(y_sem, len(line_y))
    send_all(node, size, update, returned, send_sem, recv_sem)
    rows = grid.shape[0]
    for c in range(pieces):
        spot = lax.broadcasted_iota(jnp.int32, (PIECE, rows), 0) + c * PIECE
        hot[c * PIECE : (c + 1) * PIECE, :] = jnp.where(spot == order[...], 1.0, 0.0).astype(BF16)
    for copy in copies:
        copy.wait_send()
    whole = drain(size, update, returned, send_sem, recv_sem, partner)
    whole.wait_recv()
    for c in range(pieces):
        landed[c * PIECE : (c + 1) * PIECE, :] = flat(returned, c)
    for c in range(pieces):
        here = slice(c * PIECE, (c + 1) * PIECE)
        out[here, :] = (grid[here, :].astype(F32) + dot(hot[here, :], landed[...])).astype(BF16)
    whole.wait_send()


def finish(agg, dec, outer, gain, order, grid):
    rows, width = agg.shape
    size = lax.axis_size("nodes")
    pieces = rows // PIECE
    split = pltpu.VMEM((size, rows // size, width), BF16)
    regular = pltpu.SemaphoreType.REGULAR
    return call(
        finish_kernel,
        [VMEM] * 6,
        jax.ShapeDtypeStruct(agg.shape, BF16),
        [pltpu.VMEM((rows, width), BF16), split, split, pltpu.VMEM((rows, rows), BF16), pltpu.VMEM((rows, width), BF16)]
        + [DMA((pieces,))] * 2 + [DMA] * 2 + [regular] * 2,
        collective_id=6,
        has_side_effects=True,
    )(agg, dec, outer, gain, order, grid)


def local(
    grid_latent,
    mesh_latent,
    grid_order,
    enc_send_block,
    enc_recv_block,
    enc_offsets,
    enc_classes,
    enc_live,
    mesh_send_block,
    mesh_recv_block,
    mesh_offsets,
    mesh_classes,
    mesh_live,
    dec_send_block,
    dec_recv_block,
    dec_offsets,
    dec_classes,
    dec_live,
    class_gain,
    enc_weights,
    mesh_weights,
    dec_weights,
    enc_bias,
    enc_gain,
    mesh_bias,
    mesh_gain,
    dec_bias,
    dec_gain,
):
    grid_send, grid_take, mesh_take, mesh_peer, outer, enc_gain_peer, mesh_gain_peer = start(
        grid_order, grid_latent, mesh_latent, enc_weights, mesh_weights, dec_weights, enc_gain[None, :], mesh_gain
    )
    agg = edge_sum(
        grid_send, mesh_take, enc_bias[None, :], 0, class_gain, 0,
        enc_send_block, enc_recv_block, enc_offsets, enc_classes, enc_live, 8,
    )
    mesh_own, mesh_peer, nearby, taking = refresh(
        0, True, (2,), (0,), agg, enc_weights, outer, enc_gain[None, :], enc_gain_peer, 0,
        mesh_latent, mesh_peer, mesh_weights,
    )
    for index in range(ROUNDS):
        agg = edge_sum(
            nearby, taking, mesh_bias, index, class_gain, 1,
            mesh_send_block, mesh_recv_block, mesh_offsets, mesh_classes, mesh_live, 16,
        )
        last = index == ROUNDS - 1
        mesh_own, mesh_peer, *sides = refresh(
            index + 1, not last, (index, 2), () if last else (index + 1,), agg, mesh_weights, outer,
            mesh_gain, mesh_gain_peer, index, mesh_own, mesh_peer, dec_weights if last else mesh_weights,
        )
        if not last:
            nearby, taking = sides
    (dec_send,) = sides
    agg = edge_sum(
        dec_send, grid_take, dec_bias[None, :], 0, class_gain, 2,
        dec_send_block, dec_recv_block, dec_offsets, dec_classes, dec_live, 12,
    )
    return (finish(agg, dec_weights, outer, dec_gain[None, :], grid_order, grid_latent), mesh_own)


def solution(mesh):
    in_specs = (
        P("nodes", "feat"),
        P("nodes", "feat"),
        P("nodes", None),
        P("nodes"),
        P("nodes"),
        P("nodes", None, None),
        P("nodes", None),
        P("nodes"),
        P("nodes"),
        P("nodes"),
        P("nodes", None, None),
        P("nodes", None),
        P("nodes"),
        P("nodes"),
        P("nodes"),
        P("nodes", None, None),
        P("nodes", None),
        P("nodes"),
        P(),
        P(None, None, "feat"),
        P(None, None, None, "feat"),
        P(None, None, "feat"),
        P("feat"),
        P("feat"),
        P(None, "feat"),
        P(None, "feat"),
        P("feat"),
        P("feat"),
    )
    out_specs = (P("nodes", "feat"), P("nodes", "feat"))
    return jax.shard_map(local, mesh=mesh, in_specs=in_specs, out_specs=out_specs, check_vma=False)
```

```python
import functools

import jax
import jax.numpy as jnp
from jax import lax
from jax.experimental import pallas as pl
from jax.experimental.pallas import tpu as pltpu
from jax.sharding import PartitionSpec as P

D = 512
BLOCK = 128
ROUNDS = 2
NCLASS = 8
EPS = 1e-05
F32 = jnp.float32
BF16 = jnp.bfloat16

VMEM = pl.BlockSpec(memory_space=pltpu.VMEM)
SMEM = pl.BlockSpec(memory_space=pltpu.SMEM)
HBM = pl.BlockSpec(memory_space=pltpu.HBM)
LIMIT = 20 << 20
START_LIMIT = None


def call(kernel, ins, outs, scratch=(), flops=1 << 28, out_specs=None, limit=LIMIT, **params):
    return pl.pallas_call(
        kernel,
        in_specs=ins,
        out_specs=out_specs or ([VMEM] * len(outs) if isinstance(outs, (list, tuple)) else VMEM),
        out_shape=outs,
        scratch_shapes=list(scratch),
        cost_estimate=pl.CostEstimate(flops=flops, bytes_accessed=1 << 20, transcendentals=0),
        compiler_params=pltpu.CompilerParams(vmem_limit_bytes=limit, **params),
    )


def dot(a, b, dims=((1,), (0,))):
    return lax.dot_general(a, b, (dims, ((), ())), preferred_element_type=F32)


def edge_kernel(unroll, gain_row, bias_row, send_ids, recv_ids, live, gains, offsets, labels, bias, sender, receiver, *refs):
    if len(refs) == 7:
        through, out, through_out, total, high, low, sem = refs
        passing = pltpu.make_async_copy(through, through_out, sem)
        passing.start()
    else:
        out, total, high, low = refs
        passing = None
    slots = labels.shape[0]
    blocks = total.shape[0]
    chosen = labels[...]
    weight = jnp.zeros((slots, BLOCK), F32)
    for c in range(NCLASS):
        weight = jnp.where(chosen == c, gains[gain_row, c], weight)
    alive = lax.broadcasted_iota(jnp.int32, (slots, BLOCK), 0) < live[0]
    weight = jnp.where(alive, weight, 0.0)
    top = weight.astype(BF16).astype(F32)
    high[...] = top
    low[...] = weight - top
    total[...] = jnp.zeros_like(total)
    shift = bias[bias_row : bias_row + 1, :] * 0.5
    rows = lax.broadcasted_iota(jnp.int32, (BLOCK, BLOCK), 0)

    def turn(t, carry):
        sums = []
        for u in range(unroll):
            k = t * unroll + u
            pair = offsets[k]
            from_is = rows == pair[0:1, :]
            to_is = rows == pair[1:2, :]
            hot = jnp.concatenate([jnp.where(from_is, 0.5, 0.0), jnp.where(to_is, 0.5, 0.0)], axis=0).astype(BF16)
            both = jnp.concatenate([sender[send_ids[k]], receiver[recv_ids[k]]], axis=0)
            half = dot(hot, both, ((0,), (0,))) + shift
            message = (half * (1.0 + jnp.tanh(half))).astype(BF16)
            back = jnp.concatenate(
                [jnp.where(to_is, high[pl.ds(k, 1), :], 0.0), jnp.where(to_is, low[pl.ds(k, 1), :], 0.0)], axis=1
            ).astype(BF16)
            sums.append(dot(back, jnp.concatenate([message, message], axis=0)))
        for u in range(unroll):
            taker = recv_ids[t * unroll + u]
            total[taker] = total[taker] + sums[u]
        return carry

    lax.fori_loop(0, (live[0] + unroll - 1) // unroll, turn, 0)
    for b in range(blocks):
        out[b * BLOCK : (b + 1) * BLOCK, :] = total[b].astype(BF16)
    if passing is not None:
        passing.wait()


def edge_sum(sender, receiver, bias, bias_row, gains, gain_row, send_ids, recv_ids, offsets, labels, live, unroll, through=None):
    slots = labels.shape[0]
    blocks, _, width = receiver.shape
    result = jax.ShapeDtypeStruct((blocks * BLOCK, width), BF16)
    scratch = [
        pltpu.VMEM((blocks, BLOCK, width), F32),
        pltpu.VMEM((slots, BLOCK), F32),
        pltpu.VMEM((slots, BLOCK), F32),
    ]
    kernel = functools.partial(edge_kernel, unroll, gain_row, bias_row)
    operands = (send_ids, recv_ids, live, gains, offsets, labels, bias, sender, receiver)
    specs = [SMEM] * 4 + [VMEM] * 5
    if through is None:
        return call(kernel, specs, result, scratch)(*operands)
    outs = [result, jax.ShapeDtypeStruct(through.shape, through.dtype)]
    return call(kernel, specs + [VMEM], outs, scratch + [pltpu.SemaphoreType.DMA], out_specs=[VMEM, HBM])(*operands, through)


PIECE = 256
DMA = pltpu.SemaphoreType.DMA
MESH_ID = pl.DeviceIdType.MESH


def meet(partners):
    barrier = pltpu.get_barrier_semaphore()
    for partner in partners:
        pl.semaphore_signal(barrier, inc=1, device_id=partner, device_id_type=MESH_ID)
    pl.semaphore_wait(barrier, len(partners))


def remote(source, target, send_sem, recv_sem, partner):
    return pltpu.make_async_remote_copy(
        src_ref=source, dst_ref=target, send_sem=send_sem, recv_sem=recv_sem,
        device_id=partner, device_id_type=MESH_ID,
    )


def rows_of(c, piece=PIECE):
    return pl.ds(pl.multiple_of(c * piece, piece), piece)


def ordered(matrix, feat):
    half = matrix.shape[0] // 2
    own = matrix[pl.ds(pl.multiple_of(feat * half, half), half), :]
    peer = matrix[pl.ds(pl.multiple_of((1 - feat) * half, half), half), :]
    return jnp.concatenate([own, peer], axis=0)


def put(out, c, value):
    per = value.shape[0] // BLOCK
    for i in range(per):
        out[c * per + i] = value[i * BLOCK : (i + 1) * BLOCK, :].astype(BF16)


def normed(mixed_own, mixed_peer, gain_own, gain_peer):
    total = jnp.sum(mixed_own, axis=1, keepdims=True) + jnp.sum(mixed_peer, axis=1, keepdims=True)
    square = jnp.sum(mixed_own * mixed_own, axis=1, keepdims=True) + jnp.sum(
        mixed_peer * mixed_peer, axis=1, keepdims=True
    )
    average = total * (1.0 / D)
    spread = square * (1.0 / D) - average * average
    scale = lax.rsqrt(spread + EPS)
    mine = (mixed_own - average) * scale * gain_own
    if gain_peer is None:
        return mine, None
    return mine, (mixed_peer - average) * scale * gain_peer


def exchange(own, peer, send_sems, recv_sems, partner, spots=None, piece=PIECE):
    spots = range(own.shape[0] // piece) if spots is None else spots
    return [
        remote(own.at[rows_of(s, piece)], peer.at[rows_of(s, piece)], send_sems.at[c], recv_sems.at[c], partner)
        for c, s in enumerate(spots)
    ]


def refresh_kernel(near, stage, own_at, next_at, gain_row, agg, w_own, w_peer, gain_own, gain_peer, mesh_own, mesh_peer, following, new_own, new_peer, sent, *refs):
    feat = lax.axis_index("feat")
    partner = {"feat": 1 - feat}
    if near:
        take, peer, send_sems, recv_sems, up_send, up_recv, down_send, down_recv = refs
        node, size = lax.axis_index("nodes"), lax.axis_size("nodes")
        after = {"nodes": lax.rem(node + 1, size)}
        before = {"nodes": lax.rem(node + size - 1, size)}
        meet([partner, before, after])
    else:
        peer, send_sems, recv_sems = refs
        meet([partner])
    piece = BLOCK if near else PIECE
    copies = exchange(agg, peer, send_sems, recv_sems, partner, piece=piece)
    for copy in copies:
        copy.start()
    pieces = len(copies)
    per = piece // BLOCK
    blocks = pieces * per
    shift = blocks if near else 0
    outgoing = []
    if near:
        for c in range(pieces):
            here = sent.at[pl.ds(blocks + c * per, per)]
            outgoing.append(remote(here, sent.at[pl.ds(c * per, per)], up_send.at[c], up_recv.at[c], after))
            outgoing.append(remote(here, sent.at[pl.ds(2 * blocks + c * per, per)], down_send.at[c], down_recv.at[c], before))
    mine, theirs = ordered(w_own.at[own_at], feat), ordered(w_peer.at[stage], feat)
    if not near:
        for copy in copies:
            copy.wait_recv()
    for c, copy in enumerate(copies):
        if near:
            copy.wait_recv()
        rows = rows_of(c, piece)
        both = jnp.concatenate([agg[rows, :], peer[rows, :]], axis=1)
        own, other = normed(
            dot(both, mine), dot(both, theirs), gain_own[gain_row : gain_row + 1, :], gain_peer[gain_row : gain_row + 1, :]
        )
        own = (mesh_own[rows, :].astype(F32) + own).astype(BF16)
        other = (mesh_peer[rows, :].astype(F32) + other).astype(BF16)
        new_own[rows, :] = own
        new_peer[rows, :] = other
        both = jnp.concatenate([own, other], axis=1)
        put(sent.at[pl.ds(shift, blocks)], c, dot(both, ordered(following.at[next_at + (0,)], feat)))
        if near:
            put(take, c, dot(both, ordered(following.at[next_at + (1,)], feat)))
            outgoing[2 * c].start()
            outgoing[2 * c + 1].start()
    for copy in outgoing:
        copy.wait_recv()
    for copy in copies + outgoing:
        copy.wait_send()


def refresh(stage, near, own_at, next_at, agg, w_own, w_peer, gain_own, gain_peer, gain_row, mesh_own, mesh_peer, following):
    rows, width = agg.shape
    blocks, count = rows // BLOCK, rows // (BLOCK if near else PIECE)
    shape = jax.ShapeDtypeStruct
    outs = [shape((rows, width), BF16)] * 2 + [shape((blocks * (3 if near else 1), BLOCK, width), BF16)]
    scratch = [pltpu.VMEM((rows, width), BF16), DMA((count,)), DMA((count,))]
    if near:
        outs.append(shape((blocks, BLOCK, width), BF16))
        scratch += [DMA((count,))] * 4
    return call(
        functools.partial(refresh_kernel, near, stage, own_at, next_at, gain_row),
        [VMEM] * 8,
        outs,
        scratch,
        collective_id=2 + stage,
        has_side_effects=True,
    )(agg, w_own, w_peer, gain_own, gain_peer, mesh_own, mesh_peer, following)


def extents(size):
    return (8, 4, 4) if size == 128 else (1, 2, size // 2)


def axis_peers(node, size):
    z, x, y = extents(size)
    at = (node // (x * y), (node // y) % x, node % y)
    index = lambda p: (p[0] * x + p[1]) * y + p[2]
    peers = []
    for axis, extent in enumerate((z, x, y)):
        line = []
        for step in range(1, extent):
            spot = list(at)
            spot[axis] = lax.rem(at[axis] + step, extent)
            line.append({"nodes": index(spot)})
        peers.append(line)
    return peers


def signal_all(semaphore, partners):
    for partner in partners:
        pl.semaphore_signal(semaphore, inc=1, device_id=partner, device_id_type=MESH_ID)


def send_all(node, size, source, target, send_sem, recv_sem):
    z, x, y = extents(size)

    def send(i, carry):
        j = size - i
        to_z = lax.rem(node // (x * y) + lax.rem(j, z), z)
        to_x = lax.rem((node // y) % x + lax.rem(j // z, x), x)
        to_y = lax.rem(node % y + j // (z * x), y)
        to = (to_z * x + to_x) * y + to_y
        remote(source.at[to], target.at[node], send_sem, recv_sem, {"nodes": to}).start()
        return carry

    lax.fori_loop(1, size, send, 0)
    target[pl.ds(node, 1)] = source[pl.ds(node, 1)]


def drain(ref, count, send_sem, recv_sem, partner):
    some = ref.at[pl.ds(0, count)]
    return remote(some, some, send_sem, recv_sem, partner)


def flat(ref, c):
    per = PIECE // ref.shape[1]
    return ref[pl.ds(c * per, per)].astype(F32).reshape(PIECE, ref.shape[2]).astype(BF16)


def put_split(ref, c, value):
    per = PIECE // ref.shape[1]
    ref[pl.ds(c * per, per)] = value.reshape(per, ref.shape[1], ref.shape[2]).astype(BF16)


def start_kernel(
    order, grid, own, enc, mesh_w, dec, enc_gain, mesh_gain,
    sides, takes, take, peer, outer, enc_gain_peer, mesh_gain_peer,
    picked, arrived, other, mine, near_w, load_sems, send_sems, recv_sems, grid_sends, grid_recvs, send_sem, recv_here, x_sem, y_sem,
):
    feat, node, size = lax.axis_index("feat"), lax.axis_index("nodes"), lax.axis_size("nodes")
    partner = {"feat": 1 - feat}
    line_z, line_x, line_y = axis_peers(node, size)
    barrier = pltpu.get_barrier_semaphore()
    first = [partner] + line_z + line_x + line_y
    signal_all(barrier, first)
    loads = [
        pltpu.make_async_copy(source, target, load_sems.at[i])
        for i, (source, target) in enumerate(
            [(own, mine), (enc.at[0], near_w.at[0]), (enc.at[1], near_w.at[1]), (dec.at[1], near_w.at[2])]
        )
    ]
    for load in loads:
        load.start()
    rows = grid.shape[0]
    pieces = rows // PIECE
    per = PIECE // picked.shape[1]
    spot = lax.broadcasted_iota(jnp.int32, (rows, BLOCK), 0)

    def choose(c):
        parts = []
        for h in range(PIECE // BLOCK):
            here = pl.ds(c * PIECE + h * BLOCK, BLOCK)
            hot = jnp.where(spot == order[:, here], 1.0, 0.0).astype(BF16)
            parts.append(dot(hot, grid[...], ((0,), (0,))))
        put_split(picked, c, jnp.concatenate(parts, axis=0))

    moves = [(own.at[pl.ds(c * PIECE, PIECE)], peer.at[pl.ds(c * PIECE, PIECE)]) for c in range(pieces)]
    moves += [(enc.at[2], outer.at[0])] + [(mesh_w.at[r, 2], outer.at[1 + r]) for r in range(ROUNDS)]
    moves += [(dec.at[2], outer.at[1 + ROUNDS]), (enc_gain, enc_gain_peer), (mesh_gain, mesh_gain_peer)]
    copies = [remote(s, t, send_sems.at[i], recv_sems.at[i], partner) for i, (s, t) in enumerate(moves)]

    for c in range(pieces):
        choose(c)
        if c == pieces // 2 - 1:
            pl.semaphore_wait(barrier, len(first))
            signal_all(x_sem, line_x)
            for copy in copies:
                copy.start()
        if c == pieces - 2:
            pl.semaphore_wait(x_sem, len(line_x))
            signal_all(y_sem, line_y)
    pl.semaphore_wait(y_sem, len(line_y))
    send_all(node, size, picked, arrived, send_sem, recv_here)
    for load in loads:
        load.wait()
    weight = ordered(near_w.at[1], feat)
    for c in range(pieces):
        copies[c].wait_recv()
        here = rows_of(c)
        put(take, c, dot(jnp.concatenate([mine[here, :], peer[here, :]], axis=1), weight))
    for copy in copies[pieces:]:
        copy.wait_recv()
    for copy in copies:
        copy.wait_send()
    drain(arrived, size - 1, send_sem, recv_here, partner).wait_recv()
    passes = [
        remote(arrived.at[pl.ds(c * per, per)], other.at[pl.ds(c * per, per)], grid_sends.at[c], grid_recvs.at[c], partner)
        for c in range(pieces)
    ]
    for copy in passes:
        copy.start()
    first_w, second_w = ordered(near_w.at[0], feat), ordered(near_w.at[2], feat)
    for c, copy in enumerate(passes):
        copy.wait_recv()
        both = jnp.concatenate([flat(arrived, c), flat(other, c)], axis=1)
        put(sides, c, dot(both, first_w))
        put(takes, c, dot(both, second_w))
    for copy in passes:
        copy.wait_send()
    drain(picked, size - 1, send_sem, recv_here, partner).wait_send()


def start(order, grid, own, enc, mesh_w, dec, enc_gain, mesh_gain):
    rows, width = own.shape
    size = lax.axis_size("nodes")
    count, pieces = rows // PIECE + 4 + ROUNDS, rows // PIECE
    shape = jax.ShapeDtypeStruct
    blocked = shape((rows // BLOCK, BLOCK, width), BF16)
    split = pltpu.VMEM((size, rows // size, width), BF16)
    regular = pltpu.SemaphoreType.REGULAR
    return call(
        start_kernel,
        [VMEM] * 2 + [HBM] * 6,
        [
            blocked,
            blocked,
            blocked,
            shape((rows, width), BF16),
            shape((2 + ROUNDS, D, width), BF16),
            shape((1, width), F32),
            shape((ROUNDS, width), F32),
        ],
        [split] * 3
        + [pltpu.VMEM((rows, width), BF16), pltpu.VMEM((3, D, width), BF16), DMA((4,))]
        + [DMA((count,))] * 2 + [DMA((pieces,))] * 2 + [DMA] * 2 + [regular] * 2,
        collective_id=0,
        limit=START_LIMIT,
        has_side_effects=True,
    )(order, grid, own, enc, mesh_w, dec, enc_gain, mesh_gain)


def finish_kernel(
    agg, dec, outer, gain, order, out,
    peer, update, returned, hot, landed, send_sems, recv_sems, send_sem, recv_here, x_sem, y_sem,
):
    feat, node, size = lax.axis_index("feat"), lax.axis_index("nodes"), lax.axis_size("nodes")
    partner = {"feat": 1 - feat}
    line_z, line_x, line_y = axis_peers(node, size)
    barrier = pltpu.get_barrier_semaphore()
    first = [partner] + line_z + line_x + line_y
    signal_all(barrier, first)
    pl.semaphore_wait(barrier, len(first))
    signal_all(x_sem, line_x)
    rows = agg.shape[0]
    pieces = rows // PIECE
    copies = exchange(agg, peer, send_sems, recv_sems, partner)
    for copy in copies:
        copy.start()
    mine, theirs = ordered(dec.at[2], feat), ordered(outer.at[1 + ROUNDS], feat)
    for c, copy in enumerate(copies):
        copy.wait_recv()
        here = rows_of(c)
        both = jnp.concatenate([agg[here, :], peer[here, :]], axis=1)
        fresh, _ = normed(dot(both, mine), dot(both, theirs), gain[...], None)
        put_split(update, c, fresh)
        if c == pieces // 2 - 1:
            pl.semaphore_wait(x_sem, len(line_x))
            signal_all(y_sem, line_y)
    pl.semaphore_wait(y_sem, len(line_y))
    send_all(node, size, update, returned, send_sem, recv_here)
    for c in range(pieces):
        hot_rows = lax.broadcasted_iota(jnp.int32, (PIECE, rows), 0) + c * PIECE
        hot[c * PIECE : (c + 1) * PIECE, :] = jnp.where(hot_rows == order[...], 1.0, 0.0).astype(BF16)
    for copy in copies:
        copy.wait_send()
    drain(returned, size - 1, send_sem, recv_here, partner).wait_recv()
    for c in range(pieces):
        landed[rows_of(c), :] = flat(returned, c)
    for c in range(pieces):
        here = slice(c * PIECE, (c + 1) * PIECE)
        out[here, :] = dot(hot[here, :], landed[...]).astype(BF16)
    drain(update, size - 1, send_sem, recv_here, partner).wait_send()


def finish(agg, dec, outer, gain, order):
    rows, width = agg.shape
    size = lax.axis_size("nodes")
    pieces = rows // PIECE
    split = pltpu.VMEM((size, rows // size, width), BF16)
    regular = pltpu.SemaphoreType.REGULAR
    return call(
        finish_kernel,
        [VMEM] * 5,
        jax.ShapeDtypeStruct(agg.shape, BF16),
        [pltpu.VMEM((rows, width), BF16), split, split, pltpu.VMEM((rows, rows), BF16), pltpu.VMEM((rows, width), BF16)]
        + [DMA((pieces,))] * 2 + [DMA] * 2 + [regular] * 2,
        collective_id=6,
        has_side_effects=True,
    )(agg, dec, outer, gain, order)


def local(
    grid_latent,
    mesh_latent,
    grid_order,
    enc_send_block,
    enc_recv_block,
    enc_offsets,
    enc_classes,
    enc_live,
    mesh_send_block,
    mesh_recv_block,
    mesh_offsets,
    mesh_classes,
    mesh_live,
    dec_send_block,
    dec_recv_block,
    dec_offsets,
    dec_classes,
    dec_live,
    class_gain,
    enc_weights,
    mesh_weights,
    dec_weights,
    enc_bias,
    enc_gain,
    mesh_bias,
    mesh_gain,
    dec_bias,
    dec_gain,
):
    grid_send, grid_take, mesh_take, mesh_peer, outer, enc_gain_peer, mesh_gain_peer = start(
        grid_order, grid_latent, mesh_latent, enc_weights, mesh_weights, dec_weights, enc_gain[None, :], mesh_gain
    )
    agg = edge_sum(
        grid_send, mesh_take, enc_bias[None, :], 0, class_gain, 0,
        enc_send_block, enc_recv_block, enc_offsets, enc_classes, enc_live, 8,
    )
    mesh_own, mesh_peer, nearby, taking = refresh(
        0, True, (2,), (0,), agg, enc_weights, outer, enc_gain[None, :], enc_gain_peer, 0,
        mesh_latent, mesh_peer, mesh_weights,
    )
    for index in range(ROUNDS):
        agg = edge_sum(
            nearby, taking, mesh_bias, index, class_gain, 1,
            mesh_send_block, mesh_recv_block, mesh_offsets, mesh_classes, mesh_live, 16,
        )
        last = index == ROUNDS - 1
        mesh_own, mesh_peer, *sides = refresh(
            index + 1, not last, (index, 2), () if last else (index + 1,), agg, mesh_weights, outer,
            mesh_gain, mesh_gain_peer, index, mesh_own, mesh_peer, dec_weights if last else mesh_weights,
        )
        if not last:
            nearby, taking = sides
    (dec_send,) = sides
    agg, mesh_own = edge_sum(
        dec_send, grid_take, dec_bias[None, :], 0, class_gain, 2,
        dec_send_block, dec_recv_block, dec_offsets, dec_classes, dec_live, 12, mesh_own,
    )
    placed = finish(agg, dec_weights, outer, dec_gain[None, :], grid_order)
    grid_out = (grid_latent.astype(F32) + placed.astype(F32)).astype(BF16)
    return (grid_out, mesh_own)


def solution(mesh):
    in_specs = (
        P("nodes", "feat"),
        P("nodes", "feat"),
        P("nodes", None),
        P("nodes"),
        P("nodes"),
        P("nodes", None, None),
        P("nodes", None),
        P("nodes"),
        P("nodes"),
        P("nodes"),
        P("nodes", None, None),
        P("nodes", None),
        P("nodes"),
        P("nodes"),
        P("nodes"),
        P("nodes", None, None),
        P("nodes", None),
        P("nodes"),
        P(),
        P(None, None, "feat"),
        P(None, None, None, "feat"),
        P(None, None, "feat"),
        P("feat"),
        P("feat"),
        P(None, "feat"),
        P(None, "feat"),
        P("feat"),
        P("feat"),
    )
    out_specs = (P("nodes", "feat"), P("nodes", "feat"))
    return jax.shard_map(local, mesh=mesh, in_specs=in_specs, out_specs=out_specs, check_vma=False)
```

```python
import functools

import jax
import jax.numpy as jnp
from jax import lax
from jax.experimental import pallas as pl
from jax.experimental.pallas import tpu as pltpu
from jax.sharding import PartitionSpec as P

D = 512
BLOCK = 128
ROUNDS = 2
NCLASS = 8
EPS = 1e-05
F32 = jnp.float32
BF16 = jnp.bfloat16

VMEM = pl.BlockSpec(memory_space=pltpu.VMEM)
SMEM = pl.BlockSpec(memory_space=pltpu.SMEM)
HBM = pl.BlockSpec(memory_space=pltpu.HBM)
LIMIT = 20 << 20
START_LIMIT = None


def call(kernel, ins, outs, scratch=(), flops=1 << 28, out_specs=None, limit=LIMIT, **params):
    return pl.pallas_call(
        kernel,
        in_specs=ins,
        out_specs=out_specs or ([VMEM] * len(outs) if isinstance(outs, (list, tuple)) else VMEM),
        out_shape=outs,
        scratch_shapes=list(scratch),
        cost_estimate=pl.CostEstimate(flops=flops, bytes_accessed=1 << 20, transcendentals=0),
        compiler_params=pltpu.CompilerParams(vmem_limit_bytes=limit, **params),
    )


def dot(a, b, dims=((1,), (0,))):
    return lax.dot_general(a, b, (dims, ((), ())), preferred_element_type=F32)


def edge_kernel(unroll, gain_row, bias_row, send_ids, recv_ids, live, gains, offsets, labels, bias, sender, receiver, *refs):
    if len(refs) == 7:
        through, out, through_out, total, high, low, sem = refs
        passing = pltpu.make_async_copy(through, through_out, sem)
        passing.start()
    else:
        out, total, high, low = refs
        passing = None
    slots = labels.shape[0]
    blocks = total.shape[0]
    chosen = labels[...]
    weight = jnp.zeros((slots, BLOCK), F32)
    for c in range(NCLASS):
        weight = jnp.where(chosen == c, gains[gain_row, c], weight)
    alive = lax.broadcasted_iota(jnp.int32, (slots, BLOCK), 0) < live[0]
    weight = jnp.where(alive, weight, 0.0)
    top = weight.astype(BF16).astype(F32)
    high[...] = top
    low[...] = weight - top
    total[...] = jnp.zeros_like(total)
    shift = bias[bias_row : bias_row + 1, :] * 0.5
    rows = lax.broadcasted_iota(jnp.int32, (BLOCK, BLOCK), 0)

    def turn(t, carry):
        sums = []
        for u in range(unroll):
            k = t * unroll + u
            pair = offsets[k]
            from_is = rows == pair[0:1, :]
            to_is = rows == pair[1:2, :]
            hot = jnp.concatenate([jnp.where(from_is, 0.5, 0.0), jnp.where(to_is, 0.5, 0.0)], axis=0).astype(BF16)
            both = jnp.concatenate([sender[send_ids[k]], receiver[recv_ids[k]]], axis=0)
            half = dot(hot, both, ((0,), (0,))) + shift
            message = (half * (1.0 + jnp.tanh(half))).astype(BF16)
            back = jnp.concatenate(
                [jnp.where(to_is, high[pl.ds(k, 1), :], 0.0), jnp.where(to_is, low[pl.ds(k, 1), :], 0.0)], axis=1
            ).astype(BF16)
            sums.append(dot(back, jnp.concatenate([message, message], axis=0)))
        for u in range(unroll):
            taker = recv_ids[t * unroll + u]
            total[taker] = total[taker] + sums[u]
        return carry

    lax.fori_loop(0, (live[0] + unroll - 1) // unroll, turn, 0)
    for b in range(blocks):
        out[b * BLOCK : (b + 1) * BLOCK, :] = total[b].astype(BF16)
    if passing is not None:
        passing.wait()


def edge_sum(sender, receiver, bias, bias_row, gains, gain_row, send_ids, recv_ids, offsets, labels, live, unroll, through=None):
    slots = labels.shape[0]
    blocks, _, width = receiver.shape
    result = jax.ShapeDtypeStruct((blocks * BLOCK, width), BF16)
    scratch = [
        pltpu.VMEM((blocks, BLOCK, width), F32),
        pltpu.VMEM((slots, BLOCK), F32),
        pltpu.VMEM((slots, BLOCK), F32),
    ]
    kernel = functools.partial(edge_kernel, unroll, gain_row, bias_row)
    operands = (send_ids, recv_ids, live, gains, offsets, labels, bias, sender, receiver)
    specs = [SMEM] * 4 + [VMEM] * 5
    if through is None:
        return call(kernel, specs, result, scratch)(*operands)
    outs = [result, jax.ShapeDtypeStruct(through.shape, through.dtype)]
    return call(kernel, specs + [VMEM], outs, scratch + [pltpu.SemaphoreType.DMA], out_specs=[VMEM, HBM])(*operands, through)


PIECE = 256
DMA = pltpu.SemaphoreType.DMA
MESH_ID = pl.DeviceIdType.MESH


def meet(partners):
    barrier = pltpu.get_barrier_semaphore()
    for partner in partners:
        pl.semaphore_signal(barrier, inc=1, device_id=partner, device_id_type=MESH_ID)
    pl.semaphore_wait(barrier, len(partners))


def remote(source, target, send_sem, recv_sem, partner):
    return pltpu.make_async_remote_copy(
        src_ref=source, dst_ref=target, send_sem=send_sem, recv_sem=recv_sem,
        device_id=partner, device_id_type=MESH_ID,
    )


def rows_of(c, piece=PIECE):
    return pl.ds(pl.multiple_of(c * piece, piece), piece)


def ordered(matrix, feat):
    half = matrix.shape[0] // 2
    own = matrix[pl.ds(pl.multiple_of(feat * half, half), half), :]
    peer = matrix[pl.ds(pl.multiple_of((1 - feat) * half, half), half), :]
    return jnp.concatenate([own, peer], axis=0)


def put(out, c, value):
    per = value.shape[0] // BLOCK
    for i in range(per):
        out[c * per + i] = value[i * BLOCK : (i + 1) * BLOCK, :].astype(BF16)


def normed(mixed_own, mixed_peer, gain_own, gain_peer):
    total = jnp.sum(mixed_own, axis=1, keepdims=True) + jnp.sum(mixed_peer, axis=1, keepdims=True)
    square = jnp.sum(mixed_own * mixed_own, axis=1, keepdims=True) + jnp.sum(
        mixed_peer * mixed_peer, axis=1, keepdims=True
    )
    average = total * (1.0 / D)
    spread = square * (1.0 / D) - average * average
    scale = lax.rsqrt(spread + EPS)
    mine = (mixed_own - average) * scale * gain_own
    if gain_peer is None:
        return mine, None
    return mine, (mixed_peer - average) * scale * gain_peer


def exchange(own, peer, send_sems, recv_sems, partner, spots=None, piece=PIECE):
    spots = range(own.shape[0] // piece) if spots is None else spots
    return [
        remote(own.at[rows_of(s, piece)], peer.at[rows_of(s, piece)], send_sems.at[c], recv_sems.at[c], partner)
        for c, s in enumerate(spots)
    ]


def refresh_kernel(near, stage, own_at, next_at, gain_row, agg, w_own, w_peer, gain_own, gain_peer, mesh_own, mesh_peer, following, new_own, new_peer, sent, *refs):
    feat = lax.axis_index("feat")
    partner = {"feat": 1 - feat}
    if near:
        take, peer, send_sems, recv_sems, up_send, up_recv, down_send, down_recv = refs
        node, size = lax.axis_index("nodes"), lax.axis_size("nodes")
        after = {"nodes": lax.rem(node + 1, size)}
        before = {"nodes": lax.rem(node + size - 1, size)}
        meet([partner, before, after])
    else:
        peer, send_sems, recv_sems = refs
        meet([partner])
    piece = BLOCK if near else PIECE
    copies = exchange(agg, peer, send_sems, recv_sems, partner, piece=piece)
    for copy in copies:
        copy.start()
    pieces = len(copies)
    per = piece // BLOCK
    blocks = pieces * per
    shift = blocks if near else 0
    outgoing = []
    if near:
        for c in range(pieces):
            here = sent.at[pl.ds(blocks + c * per, per)]
            outgoing.append(remote(here, sent.at[pl.ds(c * per, per)], up_send.at[c], up_recv.at[c], after))
            outgoing.append(remote(here, sent.at[pl.ds(2 * blocks + c * per, per)], down_send.at[c], down_recv.at[c], before))
    mine, theirs = ordered(w_own.at[own_at], feat), ordered(w_peer.at[stage], feat)
    if not near:
        for copy in copies:
            copy.wait_recv()
    for c, copy in enumerate(copies):
        if near:
            copy.wait_recv()
        rows = rows_of(c, piece)
        both = jnp.concatenate([agg[rows, :], peer[rows, :]], axis=1)
        own, other = normed(
            dot(both, mine), dot(both, theirs), gain_own[gain_row : gain_row + 1, :], gain_peer[gain_row : gain_row + 1, :]
        )
        own = (mesh_own[rows, :].astype(F32) + own).astype(BF16)
        other = (mesh_peer[rows, :].astype(F32) + other).astype(BF16)
        new_own[rows, :] = own
        new_peer[rows, :] = other
        both = jnp.concatenate([own, other], axis=1)
        put(sent.at[pl.ds(shift, blocks)], c, dot(both, ordered(following.at[next_at + (0,)], feat)))
        if near:
            put(take, c, dot(both, ordered(following.at[next_at + (1,)], feat)))
            outgoing[2 * c].start()
            outgoing[2 * c + 1].start()
    for copy in outgoing:
        copy.wait_recv()
    for copy in copies + outgoing:
        copy.wait_send()


def refresh(stage, near, own_at, next_at, agg, w_own, w_peer, gain_own, gain_peer, gain_row, mesh_own, mesh_peer, following):
    rows, width = agg.shape
    blocks, count = rows // BLOCK, rows // (BLOCK if near else PIECE)
    shape = jax.ShapeDtypeStruct
    outs = [shape((rows, width), BF16)] * 2 + [shape((blocks * (3 if near else 1), BLOCK, width), BF16)]
    scratch = [pltpu.VMEM((rows, width), BF16), DMA((count,)), DMA((count,))]
    if near:
        outs.append(shape((blocks, BLOCK, width), BF16))
        scratch += [DMA((count,))] * 4
    return call(
        functools.partial(refresh_kernel, near, stage, own_at, next_at, gain_row),
        [VMEM] * 8,
        outs,
        scratch,
        collective_id=2 + stage,
        has_side_effects=True,
    )(agg, w_own, w_peer, gain_own, gain_peer, mesh_own, mesh_peer, following)


def extents(size):
    return (8, 4, 4) if size == 128 else (1, 2, size // 2)


def axis_peers(node, size):
    z, x, y = extents(size)
    at = (node // (x * y), (node // y) % x, node % y)
    index = lambda p: (p[0] * x + p[1]) * y + p[2]
    peers = []
    for axis, extent in enumerate((z, x, y)):
        line = []
        for step in range(1, extent):
            spot = list(at)
            spot[axis] = lax.rem(at[axis] + step, extent)
            line.append({"nodes": index(spot)})
        peers.append(line)
    return peers


def signal_all(semaphore, partners):
    for partner in partners:
        pl.semaphore_signal(semaphore, inc=1, device_id=partner, device_id_type=MESH_ID)


def send_some(node, size, group, source, target, send_sem, recv_sem):
    z, x, y = extents(size)
    stride = (1, z, z * x)[group]
    count = (z, x, y)[group] * stride

    def send(i, carry):
        j = count - 1 - i
        to_z = lax.rem(node // (x * y) + lax.rem(j, z), z)
        to_x = lax.rem((node // y) % x + lax.rem(j // z, x), x)
        to_y = lax.rem(node % y + j // (z * x), y)
        to = (to_z * x + to_x) * y + to_y
        remote(source.at[to], target.at[node], send_sem, recv_sem, {"nodes": to}).start()
        return carry

    lax.fori_loop(0, count - stride, send, 0)


def drain(ref, count, send_sem, recv_sem, partner):
    some = ref.at[pl.ds(0, count)]
    return remote(some, some, send_sem, recv_sem, partner)


def flat(ref, c):
    per = PIECE // ref.shape[1]
    return ref[pl.ds(c * per, per)].astype(F32).reshape(PIECE, ref.shape[2]).astype(BF16)


def put_split(ref, c, value):
    per = PIECE // ref.shape[1]
    ref[pl.ds(c * per, per)] = value.reshape(per, ref.shape[1], ref.shape[2]).astype(BF16)


def start_kernel(
    order, grid, own, enc, mesh_w, dec, enc_gain, mesh_gain,
    sides, takes, take, peer, outer, enc_gain_peer, mesh_gain_peer,
    picked, arrived, other, mine, near_w, load_sems, send_sems, recv_sems, grid_sends, grid_recvs, send_sem, recv_here, x_sem, y_sem,
):
    feat, node, size = lax.axis_index("feat"), lax.axis_index("nodes"), lax.axis_size("nodes")
    partner = {"feat": 1 - feat}
    line_z, line_x, line_y = axis_peers(node, size)
    barrier = pltpu.get_barrier_semaphore()
    first = [partner] + line_z + line_x + line_y
    signal_all(barrier, first)
    loads = [
        pltpu.make_async_copy(source, target, load_sems.at[i])
        for i, (source, target) in enumerate(
            [(own, mine), (enc.at[0], near_w.at[0]), (enc.at[1], near_w.at[1]), (dec.at[1], near_w.at[2])]
        )
    ]
    for load in loads:
        load.start()
    rows = grid.shape[0]
    pieces = rows // PIECE
    per = PIECE // picked.shape[1]
    spot = lax.broadcasted_iota(jnp.int32, (rows, BLOCK), 0)

    def choose(c):
        parts = []
        for h in range(PIECE // BLOCK):
            here = pl.ds(c * PIECE + h * BLOCK, BLOCK)
            hot = jnp.where(spot == order[:, here], 1.0, 0.0).astype(BF16)
            parts.append(dot(hot, grid[...], ((0,), (0,))))
        put_split(picked, c, jnp.concatenate(parts, axis=0))

    moves = [(own.at[pl.ds(c * PIECE, PIECE)], peer.at[pl.ds(c * PIECE, PIECE)]) for c in range(pieces)]
    moves += [(enc.at[2], outer.at[0])] + [(mesh_w.at[r, 2], outer.at[1 + r]) for r in range(ROUNDS)]
    moves += [(dec.at[2], outer.at[1 + ROUNDS]), (enc_gain, enc_gain_peer), (mesh_gain, mesh_gain_peer)]
    copies = [remote(s, t, send_sems.at[i], recv_sems.at[i], partner) for i, (s, t) in enumerate(moves)]

    for c in range(pieces):
        choose(c)
    pl.semaphore_wait(barrier, len(first))
    signal_all(x_sem, line_x)
    send_some(node, size, 0, picked, arrived, send_sem, recv_here)
    for copy in copies:
        copy.start()
    pl.semaphore_wait(x_sem, len(line_x))
    signal_all(y_sem, line_y)
    send_some(node, size, 1, picked, arrived, send_sem, recv_here)
    pl.semaphore_wait(y_sem, len(line_y))
    send_some(node, size, 2, picked, arrived, send_sem, recv_here)
    arrived[pl.ds(node, 1)] = picked[pl.ds(node, 1)]
    for load in loads:
        load.wait()
    weight = ordered(near_w.at[1], feat)
    for c in range(pieces):
        copies[c].wait_recv()
        here = rows_of(c)
        put(take, c, dot(jnp.concatenate([mine[here, :], peer[here, :]], axis=1), weight))
    for copy in copies[pieces:]:
        copy.wait_recv()
    for copy in copies:
        copy.wait_send()
    drain(arrived, size - 1, send_sem, recv_here, partner).wait_recv()
    passes = [
        remote(arrived.at[pl.ds(c * per, per)], other.at[pl.ds(c * per, per)], grid_sends.at[c], grid_recvs.at[c], partner)
        for c in range(pieces)
    ]
    for copy in passes:
        copy.start()
    first_w, second_w = ordered(near_w.at[0], feat), ordered(near_w.at[2], feat)
    for copy in passes:
        copy.wait_recv()
    for c in range(pieces):
        both = jnp.concatenate([flat(arrived, c), flat(other, c)], axis=1)
        put(sides, c, dot(both, first_w))
        put(takes, c, dot(both, second_w))
    for copy in passes:
        copy.wait_send()
    drain(picked, size - 1, send_sem, recv_here, partner).wait_send()


def start(order, grid, own, enc, mesh_w, dec, enc_gain, mesh_gain):
    rows, width = own.shape
    size = lax.axis_size("nodes")
    count, pieces = rows // PIECE + 4 + ROUNDS, rows // PIECE
    shape = jax.ShapeDtypeStruct
    blocked = shape((rows // BLOCK, BLOCK, width), BF16)
    split = pltpu.VMEM((size, rows // size, width), BF16)
    regular = pltpu.SemaphoreType.REGULAR
    return call(
        start_kernel,
        [VMEM] * 2 + [HBM] * 6,
        [
            blocked,
            blocked,
            blocked,
            shape((rows, width), BF16),
            shape((2 + ROUNDS, D, width), BF16),
            shape((1, width), F32),
            shape((ROUNDS, width), F32),
        ],
        [split] * 3
        + [pltpu.VMEM((rows, width), BF16), pltpu.VMEM((3, D, width), BF16), DMA((4,))]
        + [DMA((count,))] * 2 + [DMA((pieces,))] * 2 + [DMA] * 2 + [regular] * 2,
        collective_id=0,
        limit=START_LIMIT,
        has_side_effects=True,
    )(order, grid, own, enc, mesh_w, dec, enc_gain, mesh_gain)


def finish_kernel(
    agg, dec, outer, gain, order, out,
    peer, update, returned, hot, landed, send_sems, recv_sems, send_sem, recv_here, x_sem, y_sem,
):
    feat, node, size = lax.axis_index("feat"), lax.axis_index("nodes"), lax.axis_size("nodes")
    partner = {"feat": 1 - feat}
    line_z, line_x, line_y = axis_peers(node, size)
    barrier = pltpu.get_barrier_semaphore()
    first = [partner] + line_z + line_x + line_y
    signal_all(barrier, first)
    pl.semaphore_wait(barrier, len(first))
    signal_all(x_sem, line_x)
    rows = agg.shape[0]
    pieces = rows // PIECE
    copies = exchange(agg, peer, send_sems, recv_sems, partner)
    for copy in copies:
        copy.start()
    mine, theirs = ordered(dec.at[2], feat), ordered(outer.at[1 + ROUNDS], feat)
    for copy in copies:
        copy.wait_recv()
    pl.semaphore_wait(x_sem, len(line_x))
    signal_all(y_sem, line_y)
    for c in range(pieces):
        here = rows_of(c)
        both = jnp.concatenate([agg[here, :], peer[here, :]], axis=1)
        fresh, _ = normed(dot(both, mine), dot(both, theirs), gain[...], None)
        put_split(update, c, fresh)
    send_some(node, size, 0, update, returned, send_sem, recv_here)
    send_some(node, size, 1, update, returned, send_sem, recv_here)
    pl.semaphore_wait(y_sem, len(line_y))
    send_some(node, size, 2, update, returned, send_sem, recv_here)
    returned[pl.ds(node, 1)] = update[pl.ds(node, 1)]
    for c in range(pieces):
        hot_rows = lax.broadcasted_iota(jnp.int32, (PIECE, rows), 0) + c * PIECE
        hot[c * PIECE : (c + 1) * PIECE, :] = jnp.where(hot_rows == order[...], 1.0, 0.0).astype(BF16)
    for copy in copies:
        copy.wait_send()
    drain(returned, size - 1, send_sem, recv_here, partner).wait_recv()
    for c in range(pieces):
        landed[rows_of(c), :] = flat(returned, c)
    for c in range(pieces):
        here = slice(c * PIECE, (c + 1) * PIECE)
        out[here, :] = dot(hot[here, :], landed[...]).astype(BF16)
    drain(update, size - 1, send_sem, recv_here, partner).wait_send()


def finish(agg, dec, outer, gain, order):
    rows, width = agg.shape
    size = lax.axis_size("nodes")
    pieces = rows // PIECE
    split = pltpu.VMEM((size, rows // size, width), BF16)
    regular = pltpu.SemaphoreType.REGULAR
    return call(
        finish_kernel,
        [VMEM] * 5,
        jax.ShapeDtypeStruct(agg.shape, BF16),
        [pltpu.VMEM((rows, width), BF16), split, split, pltpu.VMEM((rows, rows), BF16), pltpu.VMEM((rows, width), BF16)]
        + [DMA((pieces,))] * 2 + [DMA] * 2 + [regular] * 2,
        collective_id=6,
        has_side_effects=True,
    )(agg, dec, outer, gain, order)


def local(
    grid_latent,
    mesh_latent,
    grid_order,
    enc_send_block,
    enc_recv_block,
    enc_offsets,
    enc_classes,
    enc_live,
    mesh_send_block,
    mesh_recv_block,
    mesh_offsets,
    mesh_classes,
    mesh_live,
    dec_send_block,
    dec_recv_block,
    dec_offsets,
    dec_classes,
    dec_live,
    class_gain,
    enc_weights,
    mesh_weights,
    dec_weights,
    enc_bias,
    enc_gain,
    mesh_bias,
    mesh_gain,
    dec_bias,
    dec_gain,
):
    grid_send, grid_take, mesh_take, mesh_peer, outer, enc_gain_peer, mesh_gain_peer = start(
        grid_order, grid_latent, mesh_latent, enc_weights, mesh_weights, dec_weights, enc_gain[None, :], mesh_gain
    )
    agg = edge_sum(
        grid_send, mesh_take, enc_bias[None, :], 0, class_gain, 0,
        enc_send_block, enc_recv_block, enc_offsets, enc_classes, enc_live, 8,
    )
    mesh_own, mesh_peer, nearby, taking = refresh(
        0, True, (2,), (0,), agg, enc_weights, outer, enc_gain[None, :], enc_gain_peer, 0,
        mesh_latent, mesh_peer, mesh_weights,
    )
    for index in range(ROUNDS):
        agg = edge_sum(
            nearby, taking, mesh_bias, index, class_gain, 1,
            mesh_send_block, mesh_recv_block, mesh_offsets, mesh_classes, mesh_live, 16,
        )
        last = index == ROUNDS - 1
        mesh_own, mesh_peer, *sides = refresh(
            index + 1, not last, (index, 2), () if last else (index + 1,), agg, mesh_weights, outer,
            mesh_gain, mesh_gain_peer, index, mesh_own, mesh_peer, dec_weights if last else mesh_weights,
        )
        if not last:
            nearby, taking = sides
    (dec_send,) = sides
    agg, mesh_own = edge_sum(
        dec_send, grid_take, dec_bias[None, :], 0, class_gain, 2,
        dec_send_block, dec_recv_block, dec_offsets, dec_classes, dec_live, 12, mesh_own,
    )
    placed = finish(agg, dec_weights, outer, dec_gain[None, :], grid_order)
    grid_out = (grid_latent.astype(F32) + placed.astype(F32)).astype(BF16)
    return (grid_out, mesh_own)


def solution(mesh):
    in_specs = (
        P("nodes", "feat"),
        P("nodes", "feat"),
        P("nodes", None),
        P("nodes"),
        P("nodes"),
        P("nodes", None, None),
        P("nodes", None),
        P("nodes"),
        P("nodes"),
        P("nodes"),
        P("nodes", None, None),
        P("nodes", None),
        P("nodes"),
        P("nodes"),
        P("nodes"),
        P("nodes", None, None),
        P("nodes", None),
        P("nodes"),
        P(),
        P(None, None, "feat"),
        P(None, None, None, "feat"),
        P(None, None, "feat"),
        P("feat"),
        P("feat"),
        P(None, "feat"),
        P(None, "feat"),
        P("feat"),
        P("feat"),
    )
    out_specs = (P("nodes", "feat"), P("nodes", "feat"))
    return jax.shard_map(local, mesh=mesh, in_specs=in_specs, out_specs=out_specs, check_vma=False)
```
